32 devices in a mesh: gx: 8 (over z, x), gy: 4 (over y, core).
Axes of the slice: x: 2, y: 2, z: 4, core: 2. Of those that a mesh axis runs over, the one named last changes fastest.
Arguments:
- base_state: float32 [4, 8, 512, 512], P(None, None, 'gx', 'gy'), may hold values from -6 to 6
- base_old: float32 [4, 8, 512, 512], P(None, None, 'gx', 'gy'), may hold values from -6 to 6
- fine_state: float32 [4, 8, 8, 264, 264], P(None, None, 'gx', 'gy'), may hold values from -6 to 6
- fine_old: float32 [4, 8, 8, 264, 264], P(None, None, 'gx', 'gy'), may hold values from -6 to 6
- coupling: float32 [4, 4], replicated, may hold values from -12 to 12
- patch_offsets: int32 [8, 2], replicated, may hold values from 1 to 423, as said below
- patch_group: int32 [8], replicated, may hold values from 0 to 7, each once
Outputs:
- base_residual: float32 [4, 8, 512, 512], P(None, None, 'gx', 'gy')
- fine_residual: float32 [4, 8, 8, 264, 264], P(None, None, 'gx', 'gy')
- residual_norm: float32 [], replicated
The draws below stay inside these ranges and needn't reach their ends.
Inputs may be any that keep to these rules, and one draw needn't show every extreme that they name: `patch_offsets`: with the cycle of one base cell around it, each patch lies inside the grid, and no two patches or cycles share a cell. `patch_group`: every group owns exactly one patch.
All inputs are finite; a program needn't handle non-finite values.
Results may differ from the reference program's by a relative error of at most 0.0003.
Values sent between devices are 32-bit elements; how exact they have to be, the bound alone decides.
A program may use at most 128 MiB of HBM per device.

```python
import jax
import jax.numpy as jnp
from jax import lax

FIELDS = 4
NZ = 8
PC = 88
RATIO = 3
NX = 512
NY = 512
PATCHES = 8
FP = 264


def draw_patch_offsets(key, part):
    across = PATCHES // 4
    tile_x = NX // across
    tile_y = NY // 4
    index = jnp.arange(PATCHES, dtype=jnp.int32)
    shift_x = jax.random.randint(jax.random.fold_in(key, 11), (PATCHES,), 0, tile_x - PC - 1)
    shift_y = jax.random.randint(jax.random.fold_in(key, 23), (PATCHES,), 0, tile_y - PC - 1)
    start_x = index % across * tile_x + 1 + shift_x
    start_y = index // across * tile_y + 1 + shift_y
    order = jax.random.permutation(jax.random.fold_in(key, 37), PATCHES)
    return jnp.stack([start_x, start_y], axis=1)[order].astype(jnp.int32)


def block_scale(stream_key, shape, pieces, smallest, largest):
    factor_of = 1.0
    for dim, shards_of in pieces:
        draws = jax.random.uniform(jax.random.fold_in(jax.random.fold_in(stream_key, 6), dim), (shards_of,), jnp.float32, smallest / len(pieces), largest / len(pieces))
        factor_of = factor_of * jnp.repeat(jnp.exp(draws), shape[dim] // shards_of).reshape((-1,) + (1,) * (len(shape) - 1 - dim))
    return factor_of


def gaussian(key, shape, scale, limit, shards=(), kind=jnp.bfloat16):
    drawn = jax.random.normal(key, shape, jnp.float32) * scale
    if len(shards) > 0:
        drawn = block_scale(key, shape, shards, -0.22, 0.18) * drawn
    return jnp.clip(drawn, min=-limit, max=limit).astype(kind)


def setup_inputs(seed: int = 0) -> dict:
    key_list = jax.random.split(jax.random.key(seed), 8)
    return {
        "base_state": gaussian(key_list[0], (FIELDS, NZ, NX, NY), 1.0, 6.0, ((2, 8), (3, 4)), jnp.float32),
        "base_old": gaussian(key_list[1], (FIELDS, NZ, NX, NY), 1.0, 6.0, ((2, 8), (3, 4)), jnp.float32),
        "fine_state": gaussian(key_list[2], (FIELDS, NZ, PATCHES, FP, FP), 1.0, 6.0, ((2, 8), (3, 4)), jnp.float32),
        "fine_old": gaussian(key_list[3], (FIELDS, NZ, PATCHES, FP, FP), 1.0, 6.0, ((2, 8), (3, 4)), jnp.float32),
        "coupling": gaussian(key_list[4], (FIELDS, FIELDS), 2.0, 12.0, (), jnp.float32),
        "patch_offsets": draw_patch_offsets(jax.random.fold_in(key_list[7], 71), 0),
        "patch_group": jax.random.permutation(key_list[6], PATCHES).astype(jnp.int32),
    }


time_step = 0.1
viscosity = 0.2
vertical_mix = 0.5

def tendency(padded, state, former, coupling, inverse):
    north = padded[:, :, 2:, 1:-1]
    south = padded[:, :, :-2, 1:-1]
    east = padded[:, :, 1:-1, 2:]
    west = padded[:, :, 1:-1, :-2]
    advect = (state[0:1] * (north - south) + state[1:2] * (east - west)) * (0.5 * inverse)
    laplace = (north + south + east + west - 4.0 * state) * (inverse * inverse)
    zero_level = jnp.zeros_like(state[:, :1])
    upper = jnp.concatenate([state[:, 1:], zero_level], axis=1)
    lower = jnp.concatenate([zero_level, state[:, :-1]], axis=1)
    vertical = 2.0 * state - upper - lower
    coupled = coupling[:, 0, None, None, None] * state[0:1]
    for source in range(1, state.shape[0]):
        coupled = coupled + coupling[:, source, None, None, None] * state[source:source + 1]
    return state - former + time_step * (advect - viscosity * laplace + vertical_mix * vertical + coupled)

def reference(base_state, base_old, fine_state, fine_old, coupling, patch_offsets, patch_group):
    fields = base_state.shape[0]
    levels = base_state.shape[1]
    padded = jnp.pad(base_state, ((0, 0), (0, 0), (1, 1), (1, 1)))
    base_tend = tendency(padded, base_state, base_old, coupling, 1.0)
    owner = (patch_group[None, :] == jnp.arange(PATCHES, dtype=jnp.int32)[:, None]).astype(jnp.int32)
    placed = lax.optimization_barrier(jnp.sum(owner[:, :, None] * patch_offsets[None, :, :], axis=1)).astype(jnp.int32)
    zero = jnp.zeros((), jnp.int32)

    def one_patch(group):
        start_x = placed[group, 0]
        start_y = placed[group, 1]
        top = lax.dynamic_slice(base_state, (zero, zero, start_x - 1, start_y), (fields, levels, 1, PC))
        bottom = lax.dynamic_slice(base_state, (zero, zero, start_x + PC, start_y), (fields, levels, 1, PC))
        left = lax.dynamic_slice(base_state, (zero, zero, start_x, start_y - 1), (fields, levels, PC, 1))
        right = lax.dynamic_slice(base_state, (zero, zero, start_x, start_y + PC), (fields, levels, PC, 1))
        top = jnp.repeat(top, RATIO, axis=3)
        bottom = jnp.repeat(bottom, RATIO, axis=3)
        left = jnp.repeat(left, RATIO, axis=2)
        right = jnp.repeat(right, RATIO, axis=2)
        state = lax.dynamic_index_in_dim(fine_state, group, 2, keepdims=False)
        former = lax.dynamic_index_in_dim(fine_old, group, 2, keepdims=False)
        corner = jnp.zeros((fields, levels, 1, 1), jnp.float32)
        top_row = jnp.concatenate([corner, top, corner], axis=3)
        bottom_row = jnp.concatenate([corner, bottom, corner], axis=3)
        middle = jnp.concatenate([left, state, right], axis=3)
        padded_fine = jnp.concatenate([top_row, middle, bottom_row], axis=2)
        result = tendency(padded_fine, state, former, coupling, float(RATIO))
        coarse = result.reshape(fields, levels, PC, RATIO, PC, RATIO).mean(axis=(3, 5))
        return (result, coarse)
    fine_res, restricted = lax.map(one_patch, jnp.arange(PATCHES, dtype=jnp.int32))
    fine_res = jnp.moveaxis(fine_res, 0, 2)

    def place(group, carry):
        merged, covered = carry
        start = (zero, zero, placed[group, 0], placed[group, 1])
        merged = lax.dynamic_update_slice(merged, restricted[group], start)
        covered = lax.dynamic_update_slice(covered, jnp.ones((1, 1, PC, PC), jnp.float32), start)
        return (merged, covered)
    covered_init = jnp.zeros((1, 1, base_state.shape[2], base_state.shape[3]), jnp.float32)
    merged, covered = lax.fori_loop(0, PATCHES, place, (base_tend, covered_init))
    base_sq = jnp.sum(jnp.where(covered > 0.5, 0.0, base_tend * base_tend))
    fine_sq = jnp.sum(fine_res * fine_res) / (RATIO * RATIO)
    residual_norm = jnp.sqrt(base_sq + fine_sq)
    return (merged, fine_res, residual_norm)
```

```python
import functools

import jax
import jax.numpy as jnp
from jax import lax
from jax.experimental import pallas as pl
from jax.experimental.pallas import tpu as pltpu
from jax.sharding import PartitionSpec as P

PC = 88
RATIO = 3

time_step = 0.1
viscosity = 0.2
vertical_mix = 0.5

F32 = jnp.float32
BF16 = jnp.bfloat16
HIGH = lax.Precision.HIGHEST
MESH = pl.DeviceIdType.MESH
VMEM = pl.BlockSpec(memory_space=pltpu.VMEM)
SMEM = pl.BlockSpec(memory_space=pltpu.SMEM)


def params(**more):
    return pltpu.CompilerParams(vmem_limit_bytes=58 * 1024 * 1024, **more)


def iota(shape, dim):
    return lax.broadcasted_iota(jnp.int32, shape, dim)


def comm_kernel(plan, axes, inner, *refs):
    count = len(plan)
    sources, targets = refs[:count], refs[count : 2 * count]
    send_sem, recv_sem, local_sem = refs[2 * count :]
    barrier = pltpu.get_barrier_semaphore()
    total = 0
    for axis, size in axes.items():
        me = lax.axis_index(axis)
        for step in range(1, size):
            pl.semaphore_signal(
                barrier, inc=1, device_id={axis: lax.rem(me + step, size)}, device_id_type=MESH
            )
        total += size - 1
    pl.semaphore_wait(barrier, total)
    used = [0]
    waiting = []

    def send(source, target, axis, peer):
        slot = used[0]
        used[0] += 1
        copy = pltpu.make_async_remote_copy(
            src_ref=source,
            dst_ref=target,
            send_sem=send_sem.at[slot],
            recv_sem=recv_sem.at[slot],
            device_id={axis: peer},
            device_id_type=MESH,
        )
        copy.start()
        return copy

    relays = []
    local = []
    for index, (mode, axis) in enumerate(plan):
        source, target = sources[index], targets[index]
        size = axes[axis]
        me = lax.axis_index(axis)
        if mode == "shift":
            up, down = lax.rem(me + 1, size), lax.rem(me + size - 1, size)
            waiting.append(send(source.at[1], target.at[0], axis, up))
            waiting.append(send(source.at[0], target.at[1], axis, down))
            continue
        own = pltpu.make_async_copy(
            source.at[me] if mode == "exchange" else source, target.at[me], local_sem.at[index]
        )
        own.start()
        local.append(own)
        if mode == "relay":
            outer = size // inner
            high, low = lax.div(me, inner), lax.rem(me, inner)
            for step in range(1, outer):
                peer = lax.rem(high + step, outer) * inner + low
                origin = lax.rem(high + outer - step, outer) * inner + low
                relays.append((send(source, target.at[me], axis, peer), target, origin))
            for hop in range(1, inner):
                peer = high * inner + lax.rem(low + hop, inner)
                waiting.append(send(source, target.at[me], axis, peer))
            continue
        for step in range(1, size):
            peer = lax.rem(me + step, size)
            part = source.at[peer] if mode == "exchange" else source
            waiting.append(send(part, target.at[me], axis, peer))
    for copy, target, origin in relays:
        copy.wait_recv()
        me = lax.axis_index("gx")
        high, low = lax.div(me, inner), lax.rem(me, inner)
        for hop in range(1, inner):
            peer = high * inner + lax.rem(low + hop, inner)
            waiting.append(send(target.at[origin], target.at[origin], "gx", peer))
    for copy, _, _ in relays:
        copy.wait_send()
    for copy in waiting:
        copy.wait()
    for copy in local:
        copy.wait()


def communicate(name, ident, sizes, plan, *arrays):
    axes = {axis: sizes[axis] for _, axis in plan}
    inner = 1
    while (2 * inner) ** 2 <= sizes["gx"]:
        inner *= 2
    slots = 0
    shapes = []
    for (mode, axis), array in zip(plan, arrays):
        size = axes[axis]
        if mode == "shift":
            slots += 2
            shapes.append(array.shape)
        elif mode == "exchange":
            slots += size - 1
            shapes.append(array.shape)
        else:
            slots += size - 1
            shapes.append((size, *array.shape))
    return pl.pallas_call(
        functools.partial(comm_kernel, plan, axes, inner),
        out_shape=[jax.ShapeDtypeStruct(s, F32) for s in shapes],
        in_specs=[VMEM] * len(plan),
        out_specs=[VMEM] * len(plan),
        scratch_shapes=[
            pltpu.SemaphoreType.DMA((slots,)),
            pltpu.SemaphoreType.DMA((slots,)),
            pltpu.SemaphoreType.DMA((len(plan),)),
        ],
        compiler_params=params(collective_id=ident, has_side_effects=True),
        name=name,
    )(*arrays)


def prepare_kernel(groups, last_row, rows_ref, cols_ref, base, top, bottom, cyc, brow, bcol, frow):
    fields, levels, block_x, block_y = base.shape
    pick_rows = (iota((2 * groups, block_x), 1) == rows_ref[...]).astype(F32)
    pick_cols = (iota((2 * groups + 8, block_y), 1) == cols_ref[...]).astype(F32)
    for z in range(levels):
        for f in range(fields):
            q = base[f, z]
            flat = z * fields + f
            found = jnp.dot(pick_rows, q, precision=HIGH, preferred_element_type=F32)
            side = lax.dot_general(
                pick_cols, q, (((1,), (1,)), ((), ())), precision=HIGH, preferred_element_type=F32
            )
            both = jnp.concatenate([side[:groups], side[groups : 2 * groups]], axis=1)
            for g in range(groups):
                high = z * 2 * fields + f
                cyc[g, high : high + 1] = found[g : g + 1]
                cyc[g, high + fields : high + fields + 1] = found[groups + g : groups + g + 1]
                at = 2 * fields * levels + flat
                cyc[g, at : at + 1] = both[g : g + 1]
            brow[0, flat : flat + 1] = q[:1]
            brow[1, flat : flat + 1] = q[block_x - 1 :]
            bcol[0, flat : flat + 1] = side[2 * groups : 2 * groups + 1]
            bcol[1, flat : flat + 1] = side[2 * groups + 1 : 2 * groups + 2]
            frow[0, flat : flat + 1] = top[f, z, 0, :1]
            frow[1, flat : flat + 1] = bottom[f, z, 0, last_row : last_row + 1]


def cycle_kernel(groups, fields, block_x, meta, got, piece):
    half = got.shape[1] * 2 // 3
    width = got.shape[2]
    row_block = meta[2 * groups]
    start = meta[2 * row_block]
    rows = got[0, :half]
    sides = None
    for b in range(groups):
        if b:
            rows = rows + got[b, :half]
        lane = iota((width, 2 * width), 0)
        slot = iota((width, 2 * width), 1)
        low = (lane < block_x) & (lane + b * block_x == slot + start) & (slot < PC)
        high = (
            (lane >= block_x)
            & (lane - block_x + b * block_x == slot - width + start)
            & (slot >= width)
            & (slot < width + PC)
        )
        term = jnp.dot(
            got[b, half:], (low | high).astype(F32), precision=HIGH, preferred_element_type=F32
        )
        sides = term if sides is None else sides + term
    piece[:half] = rows
    for z in range(half // (2 * fields)):
        at = half + z * 2 * fields
        piece[at : at + fields] = sides[z * fields : (z + 1) * fields, :width]
        piece[at + fields : at + 2 * fields] = sides[z * fields : (z + 1) * fields, width:]


def level(state, former, coupling, z, first, last, left, right, inverse):
    fields, levels = len(first), state(None, None)
    q = [state(f, z) for f in range(fields)]
    out = []
    for f in range(fields):
        north = jnp.concatenate([q[f][1:], last[f]], axis=0)
        south = jnp.concatenate([first[f], q[f][:-1]], axis=0)
        east = jnp.concatenate([q[f][:, 1:], right[f]], axis=1)
        west = jnp.concatenate([left[f], q[f][:, :-1]], axis=1)
        advect = (q[0] * (north - south) + q[1] * (east - west)) * (0.5 * inverse)
        laplace = (north + south + east + west - 4.0 * q[f]) * (inverse * inverse)
        upper = jnp.where(z < levels - 1, state(f, jnp.minimum(z + 1, levels - 1)), 0.0)
        lower = jnp.where(z > 0, state(f, jnp.maximum(z - 1, 0)), 0.0)
        vertical = 2.0 * q[f] - upper - lower
        coupled = coupling[f, 0] * q[0]
        for g in range(1, fields):
            coupled = coupled + coupling[f, g] * q[g]
        out.append(
            q[f]
            - former(f)
            + time_step * (advect - viscosity * laplace + vertical_mix * vertical + coupled)
        )
    return out


def fold(values):
    total = jnp.sum(values, axis=0, keepdims=True)
    acc = total[:, :128]
    for at in range(128, values.shape[1], 128):
        part = total[:, at : at + 128]
        if part.shape[1] < 128:
            part = jnp.concatenate([part, jnp.zeros((1, 128 - part.shape[1]), F32)], axis=1)
        acc = acc + part
    return acc


def fine_kernel(
    groups, members, meta, coupling, gath, halo, state, old, res, rest, sq, edge, side, fit, thin
):
    z = pl.program_id(0)
    fields, levels = state.shape[:2]
    fine_rows, fine_cols = state.shape[3:]
    piece = fine_rows // RATIO
    block_y = gath.shape[2]
    row_block = meta[2 * groups]
    col_block = meta[2 * groups + 1]
    start_y = meta[2 * row_block + 1]
    half = 2 * fields * levels

    @pl.when(z == 0)
    def _():
        sq[...] = jnp.zeros_like(sq)
        lane = iota((block_y, fine_cols), 0)
        fine = iota((block_y, fine_cols), 1) // RATIO
        rows = None
        cols = gath[0, half:]
        for b in range(members):
            pick = (lane + b * block_y == fine + start_y).astype(F32)
            term = jnp.dot(gath[b, :half], pick, precision=HIGH, preferred_element_type=F32)
            rows = term if rows is None else rows + term
            if b:
                cols = cols + gath[b, half:]
        edge[...] = rows
        pick = iota((128, 128), 0) == piece * col_block + iota((128, 128), 1) // RATIO
        side[...] = jnp.dot(cols, pick.astype(F32), precision=HIGH, preferred_element_type=F32)
        cell = iota((fine_cols, 128), 0) // RATIO + start_y
        fit[...] = (lax.rem(cell, block_y) == iota((fine_cols, 128), 1)).astype(F32).astype(BF16)

    at = pl.multiple_of(z * 2 * fields, 8)
    edges = edge[pl.ds(at, 2 * fields)]
    turned = jnp.transpose(side[pl.ds(at, 2 * fields)])
    first, last, left, right = [], [], [], []
    for f in range(fields):
        above = halo[0, pl.ds(z * fields + f, 1)]
        below = halo[1, pl.ds(z * fields + f, 1)]
        first.append(jnp.where(col_block == 0, edges[f : f + 1], above))
        last.append(jnp.where(col_block == members - 1, edges[fields + f : fields + f + 1], below))
        left.append(turned[:fine_rows, f : f + 1])
        right.append(turned[:fine_rows, fields + f : fields + f + 1])

    def cell(f, at):
        return levels if f is None else state[f, at, 0]

    got = level(
        cell, lambda f: old[f, 0, 0], coupling, z, first, last, left, right, float(RATIO)
    )
    squares = None
    for f in range(fields):
        res[f, 0, 0] = got[f]
        squares = got[f] * got[f] if f == 0 else squares + got[f] * got[f]
        major = got[f].astype(BF16)
        minor = (got[f] - major.astype(F32)).astype(BF16)
        narrow = jnp.dot(major, fit[...], preferred_element_type=F32) + jnp.dot(
            minor, fit[...], preferred_element_type=F32
        )
        thin[f] = narrow * (1.0 / (RATIO * RATIO))
        total = thin[f, pl.ds(0, piece, stride=RATIO), :]
        for k in range(1, RATIO):
            total = total + thin[f, pl.ds(k, piece, stride=RATIO), :]
        rest[f, pl.ds(z, piece, stride=levels), :] = total
    sq[0:1] += fold(squares) * (1.0 / (RATIO * RATIO))


def base_kernel(groups, members, meta, coupling, rows, cols, state, old, res, sq):
    z = pl.program_id(0)
    fields, levels, block_x, block_y = state.shape
    row_block = meta[2 * groups]
    col_block = meta[2 * groups + 1]

    @pl.when(z == 0)
    def _():
        sq[...] = jnp.zeros_like(sq)

    first, last, left, right = [], [], [], []
    for f in range(fields):
        at = z * fields + f
        first.append(jnp.where(row_block > 0, rows[0, pl.ds(at, 1)], 0.0))
        last.append(jnp.where(row_block < groups - 1, rows[1, pl.ds(at, 1)], 0.0))
        left.append(jnp.where(col_block > 0, cols[0, pl.ds(at, 1)], 0.0))
        right.append(jnp.where(col_block < members - 1, cols[1, pl.ds(at, 1)], 0.0))
    turned = jnp.transpose(jnp.concatenate(left + right, axis=0))
    left = [turned[:, f : f + 1] for f in range(fields)]
    right = [turned[:, fields + f : fields + f + 1] for f in range(fields)]

    def cell(f, at):
        return levels if f is None else state[f, at]

    got = level(cell, lambda f: old[f, 0], coupling, z, first, last, left, right, 1.0)
    x = iota((block_x, block_y), 0) + row_block * block_x
    y = iota((block_x, block_y), 1) + col_block * block_y
    covered = jnp.zeros((block_x, block_y), jnp.bool_)
    for g in range(groups):
        dx, dy = x - meta[2 * g], y - meta[2 * g + 1]
        covered = covered | ((dx >= 0) & (dx < PC) & (dy >= 0) & (dy < PC))
    squares = None
    for f in range(fields):
        res[f, 0] = got[f]
        squares = got[f] * got[f] if f == 0 else squares + got[f] * got[f]
    sq[0:1] += fold(jnp.where(covered, 0.0, squares))


def sort_kernel(groups, members, block_x, meta, got, sums, slots, total):
    fields, depth, block_y = got.shape[1:]
    levels = depth * RATIO // (PC * RATIO // members)
    piece = depth // levels
    row_block = meta[2 * groups]
    col_block = meta[2 * groups + 1]
    acc = sums[0]
    for g in range(1, groups):
        acc = acc + sums[g]
    total[...] = acc
    for g in range(groups):
        begin = meta[2 * g] + col_block * piece - row_block * block_x
        start_y = meta[2 * g + 1]
        here = (begin < block_x) & (begin + piece > 0)
        for b in range(members):
            shift = start_y - b * block_y

            @pl.when(here & (shift < block_y) & (shift + PC > 0))
            def _():
                lane = iota((depth, block_y), 1)
                inside = (lane >= shift) & (lane < shift + PC)
                for f in range(fields):
                    slots[b, f] = jnp.where(inside, got[g, f], slots[b, f])


def place_kernel(groups, members, meta, tend, got, sums, out, norm, laid):
    fields, levels, block_x, block_y = tend.shape
    depth = got.shape[2]
    piece = depth // levels
    row_block = meta[2 * groups]
    col_block = meta[2 * groups + 1]
    acc = sums[0]
    for b in range(1, members):
        acc = acc + sums[b]
    norm[...] = jnp.sqrt(jnp.sum(acc, keepdims=True))
    x = iota((block_x, block_y), 0) + row_block * block_x
    y = iota((block_x, block_y), 1) + col_block * block_y
    covered = jnp.zeros((block_x, block_y), jnp.bool_)
    for g in range(groups):
        dx, dy = x - meta[2 * g], y - meta[2 * g + 1]
        covered = covered | ((dx >= 0) & (dx < PC) & (dy >= 0) & (dy < PC))
        begin = meta[2 * g] - row_block * block_x
        shift = meta[2 * g + 1] - col_block * block_y

        @pl.when((begin < block_x) & (begin + PC > 0) & (shift < block_y) & (shift + PC > 0))
        def _():
            lane = iota((levels, block_y), 1)
            inside = (lane >= shift) & (lane < shift + PC)

            def row(at, carry):
                patch_row = at - begin
                part = patch_row // piece
                source = pl.multiple_of((patch_row - part * piece) * levels, levels)
                target = pl.multiple_of(at * levels, levels)
                for f in range(fields):
                    laid[f, pl.ds(target, levels)] = jnp.where(
                        inside,
                        got[part, f, pl.ds(source, levels)],
                        laid[f, pl.ds(target, levels)],
                    )
                return carry

            lax.fori_loop(jnp.maximum(begin, 0), jnp.minimum(begin + PC, block_x), row, 0)

    for f in range(fields):
        for z in range(levels):
            out[f, z] = jnp.where(
                covered, laid[f, pl.ds(z, block_x, stride=levels), :], tend[f, z]
            )


def local(sizes, base_state, base_old, fine_state, fine_old, coupling, patch_offsets, patch_group):
    groups, members = sizes["gx"], sizes["gy"]
    row_block = lax.axis_index("gx")
    col_block = lax.axis_index("gy")
    fields, levels, block_x, block_y = base_state.shape
    fine_rows, fine_cols = fine_state.shape[3:]
    piece = fine_rows // RATIO
    flat = fields * levels
    owner = (patch_group[None, :] == jnp.arange(groups, dtype=jnp.int32)[:, None]).astype(jnp.int32)
    placed = jnp.sum(owner[:, :, None] * patch_offsets[None, :, :], axis=1)
    meta = jnp.concatenate([placed.reshape(-1), jnp.stack([row_block, col_block])])
    row_pick = jnp.concatenate([placed[:, 0] - 1, placed[:, 0] + PC]) - row_block * block_x
    col_pick = jnp.concatenate([placed[:, 1] - 1, placed[:, 1] + PC]) - col_block * block_y
    ends = jnp.array([0, block_y - 1, -1, -1, -1, -1, -1, -1], jnp.int32)
    col_pick = jnp.concatenate([col_pick, ends])

    def shape(*dims):
        return jax.ShapeDtypeStruct(dims, F32)

    tail = fine_rows - 1
    cyc, brow, bcol, frow = pl.pallas_call(
        functools.partial(prepare_kernel, groups, tail % 8),
        grid=(1,),
        out_shape=[
            shape(groups, 3 * flat, block_y),
            shape(2, flat, block_y),
            shape(2, flat, block_x),
            shape(2, flat, fine_cols),
        ],
        in_specs=[
            VMEM,
            VMEM,
            VMEM,
            pl.BlockSpec((fields, levels, 1, 8, fine_cols), lambda i: (0, 0, 0, 0, 0)),
            pl.BlockSpec((fields, levels, 1, 8, fine_cols), lambda i: (0, 0, 0, tail // 8, 0)),
        ],
        out_specs=[VMEM] * 4,
        compiler_params=params(),
        name="prepare",
    )(row_pick[:, None], col_pick[:, None], base_state, fine_state, fine_state)

    cyc, brow, bcol, frow = communicate(
        "edges",
        1,
        sizes,
        (("exchange", "gx"), ("shift", "gx"), ("shift", "gy"), ("shift", "gy")),
        cyc,
        brow,
        bcol,
        frow,
    )
    cycle = pl.pallas_call(
        functools.partial(cycle_kernel, groups, fields, block_x),
        out_shape=shape(4 * flat, block_y),
        in_specs=[SMEM, VMEM],
        out_specs=VMEM,
        compiler_params=params(),
        name="cycle",
    )(meta, cyc)
    (gath,) = communicate("members", 2, sizes, (("gather", "gy"),), cycle)

    slab = (fields, levels, 1, fine_rows, fine_cols)
    thin = (fields, 1, 1, fine_rows, fine_cols)
    fine_res, rest, fine_sq = pl.pallas_call(
        functools.partial(fine_kernel, groups, members),
        grid=(levels,),
        out_shape=[shape(*slab), shape(fields, piece * levels, 128), shape(8, 128)],
        in_specs=[
            SMEM,
            SMEM,
            VMEM,
            VMEM,
            pl.BlockSpec(slab, lambda z: (0, 0, 0, 0, 0)),
            pl.BlockSpec(thin, lambda z: (0, z, 0, 0, 0)),
        ],
        out_specs=[
            pl.BlockSpec(thin, lambda z: (0, z, 0, 0, 0)),
            pl.BlockSpec((fields, piece * levels, 128), lambda z: (0, 0, 0)),
            pl.BlockSpec((8, 128), lambda z: (0, 0)),
        ],
        scratch_shapes=[
            pltpu.VMEM((2 * flat, fine_cols), F32),
            pltpu.VMEM((2 * flat, 128), F32),
            pltpu.VMEM((fine_cols, 128), BF16),
            pltpu.VMEM((fields, fine_rows, 128), F32),
        ],
        compiler_params=params(),
        name="fine",
    )(meta, coupling, gath, frow, fine_state, fine_old)

    whole = (fields, levels, block_x, block_y)
    sheet = (fields, 1, block_x, block_y)
    tend, base_sq = pl.pallas_call(
        functools.partial(base_kernel, groups, members),
        grid=(levels,),
        out_shape=[shape(*whole), shape(8, 128)],
        in_specs=[
            SMEM,
            SMEM,
            VMEM,
            VMEM,
            pl.BlockSpec(whole, lambda z: (0, 0, 0, 0)),
            pl.BlockSpec(sheet, lambda z: (0, z, 0, 0)),
        ],
        out_specs=[
            pl.BlockSpec(sheet, lambda z: (0, z, 0, 0)),
            pl.BlockSpec((8, 128), lambda z: (0, 0)),
        ],
        compiler_params=params(),
        name="base",
    )(meta, coupling, brow, bcol, base_state, base_old)

    gathered, sums = communicate(
        "owners", 3, sizes, (("relay", "gx"), ("gather", "gx")), rest, fine_sq + base_sq
    )
    slots, total = pl.pallas_call(
        functools.partial(sort_kernel, groups, members, block_x),
        out_shape=[shape(members, fields, piece * levels, block_y), shape(8, 128)],
        in_specs=[SMEM, VMEM, VMEM],
        out_specs=[VMEM, VMEM],
        compiler_params=params(),
        name="sort",
    )(meta, gathered, sums)
    slots, sums = communicate(
        "columns", 4, sizes, (("exchange", "gy"), ("gather", "gy")), slots, total
    )
    base_out, norm = pl.pallas_call(
        functools.partial(place_kernel, groups, members),
        out_shape=[shape(*whole), shape(1, 1)],
        in_specs=[SMEM, VMEM, VMEM, VMEM],
        out_specs=[VMEM, VMEM],
        scratch_shapes=[pltpu.VMEM((fields, block_x * levels, block_y), F32)],
        compiler_params=params(),
        name="place",
    )(meta, tend, slots, sums)
    return (base_out, fine_res, norm[0, 0])


def solution(mesh):
    placed = (
        P(None, None, "gx", "gy"),
        P(None, None, "gx", "gy"),
        P(None, None, "gx", "gy", None),
        P(None, None, "gx", "gy", None),
        P(),
        P(),
        P(),
    )
    return jax.shard_map(
        functools.partial(local, dict(mesh.shape)),
        mesh=mesh,
        in_specs=placed,
        out_specs=(P(None, None, "gx", "gy"), P(None, None, "gx", "gy", None), P()),
        check_vma=False,
    )
```

```python
import functools

import jax
import jax.numpy as jnp
from jax import lax
from jax.experimental import pallas as pl
from jax.experimental.pallas import tpu as pltpu
from jax.sharding import PartitionSpec as P

PC = 88
RATIO = 3

time_step = 0.1
viscosity = 0.2
vertical_mix = 0.5

F32 = jnp.float32
BF16 = jnp.bfloat16
HIGH = lax.Precision.HIGHEST
MESH = pl.DeviceIdType.MESH
VMEM = pl.BlockSpec(memory_space=pltpu.VMEM)
SMEM = pl.BlockSpec(memory_space=pltpu.SMEM)


def params(**more):
    return pltpu.CompilerParams(vmem_limit_bytes=58 * 1024 * 1024, **more)


def iota(shape, dim):
    return lax.broadcasted_iota(jnp.int32, shape, dim)


def comm_kernel(plan, axes, inner, *refs):
    count = len(plan)
    sources, targets = refs[:count], refs[count : 2 * count]
    send_sem, recv_sem, local_sem = refs[2 * count :]
    barrier = pltpu.get_barrier_semaphore()
    total = 0
    for axis, size in axes.items():
        me = lax.axis_index(axis)
        for step in range(1, size):
            pl.semaphore_signal(
                barrier, inc=1, device_id={axis: lax.rem(me + step, size)}, device_id_type=MESH
            )
        total += size - 1
    pl.semaphore_wait(barrier, total)
    used = [0]
    waiting = []

    def send(source, target, axis, peer):
        slot = used[0]
        used[0] += 1
        copy = pltpu.make_async_remote_copy(
            src_ref=source,
            dst_ref=target,
            send_sem=send_sem.at[slot],
            recv_sem=recv_sem.at[slot],
            device_id={axis: peer},
            device_id_type=MESH,
        )
        copy.start()
        return copy

    relays = []
    local = []
    for index, (mode, axis) in enumerate(plan):
        source, target = sources[index], targets[index]
        size = axes[axis]
        me = lax.axis_index(axis)
        if mode == "shift":
            up, down = lax.rem(me + 1, size), lax.rem(me + size - 1, size)
            waiting.append(send(source.at[1], target.at[0], axis, up))
            waiting.append(send(source.at[0], target.at[1], axis, down))
            continue
        own = pltpu.make_async_copy(
            source.at[me] if mode == "exchange" else source, target.at[me], local_sem.at[index]
        )
        own.start()
        local.append(own)
        if mode == "relay":
            outer = size // inner
            high, low = lax.div(me, inner), lax.rem(me, inner)
            for step in range(1, outer):
                peer = lax.rem(high + step, outer) * inner + low
                origin = lax.rem(high + outer - step, outer) * inner + low
                relays.append((send(source, target.at[me], axis, peer), target, origin))
            for hop in range(1, inner):
                peer = high * inner + lax.rem(low + hop, inner)
                waiting.append(send(source, target.at[me], axis, peer))
            continue
        for step in range(1, size):
            peer = lax.rem(me + step, size)
            part = source.at[peer] if mode == "exchange" else source
            waiting.append(send(part, target.at[me], axis, peer))
    for copy, target, origin in relays:
        copy.wait_recv()
        me = lax.axis_index("gx")
        high, low = lax.div(me, inner), lax.rem(me, inner)
        for hop in range(1, inner):
            peer = high * inner + lax.rem(low + hop, inner)
            waiting.append(send(target.at[origin], target.at[origin], "gx", peer))
    for copy, _, _ in relays:
        copy.wait_send()
    for copy in waiting:
        copy.wait()
    for copy in local:
        copy.wait()


def communicate(name, ident, sizes, plan, *arrays):
    axes = {axis: sizes[axis] for _, axis in plan}
    inner = 1
    while (2 * inner) ** 2 <= sizes["gx"]:
        inner *= 2
    slots = 0
    shapes = []
    for (mode, axis), array in zip(plan, arrays):
        size = axes[axis]
        if mode == "shift":
            slots += 2
            shapes.append(array.shape)
        elif mode == "exchange":
            slots += size - 1
            shapes.append(array.shape)
        else:
            slots += size - 1
            shapes.append((size, *array.shape))
    return pl.pallas_call(
        functools.partial(comm_kernel, plan, axes, inner),
        out_shape=[jax.ShapeDtypeStruct(s, F32) for s in shapes],
        in_specs=[VMEM] * len(plan),
        out_specs=[VMEM] * len(plan),
        scratch_shapes=[
            pltpu.SemaphoreType.DMA((slots,)),
            pltpu.SemaphoreType.DMA((slots,)),
            pltpu.SemaphoreType.DMA((len(plan),)),
        ],
        compiler_params=params(collective_id=ident, has_side_effects=True),
        name=name,
    )(*arrays)


def prepare_kernel(groups, offsets, owners, base, top, bottom, cyc, brow, bcol, frow, meta):
    fields, levels, block_x, block_y = base.shape
    row_block = lax.axis_index("gx")
    col_block = lax.axis_index("gy")
    meta[2 * groups] = row_block
    meta[2 * groups + 1] = col_block
    row_pick = jnp.full((2 * groups, block_x), -1, jnp.int32)
    col_pick = jnp.full((2 * groups + 8, block_y), -1, jnp.int32)
    row_slot = iota(row_pick.shape, 0)
    col_slot = iota(col_pick.shape, 0)
    for p in range(groups):
        g = owners[p]
        meta[2 * g] = offsets[p, 0]
        meta[2 * g + 1] = offsets[p, 1]
        row = offsets[p, 0] - row_block * block_x
        col = offsets[p, 1] - col_block * block_y
        row_pick = jnp.where(row_slot == g, row - 1, row_pick)
        row_pick = jnp.where(row_slot == g + groups, row + PC, row_pick)
        col_pick = jnp.where(col_slot == g, col - 1, col_pick)
        col_pick = jnp.where(col_slot == g + groups, col + PC, col_pick)
    col_pick = jnp.where(col_slot == 2 * groups, 0, col_pick)
    col_pick = jnp.where(col_slot == 2 * groups + 1, block_y - 1, col_pick)
    pick_rows = (iota(row_pick.shape, 1) == row_pick).astype(F32)
    pick_cols = (iota(col_pick.shape, 1) == col_pick).astype(F32)
    for z in range(levels):
        for f in range(fields):
            q = base[f, z]
            flat = z * fields + f
            found = jnp.dot(pick_rows, q, precision=HIGH, preferred_element_type=F32)
            side = lax.dot_general(
                pick_cols, q, (((1,), (1,)), ((), ())), precision=HIGH, preferred_element_type=F32
            )
            both = jnp.concatenate([side[:groups], side[groups : 2 * groups]], axis=1)
            for g in range(groups):
                high = z * 2 * fields + f
                cyc[g, high : high + 1] = found[g : g + 1]
                cyc[g, high + fields : high + fields + 1] = found[groups + g : groups + g + 1]
                at = 2 * fields * levels + flat
                cyc[g, at : at + 1] = both[g : g + 1]
            brow[0, flat : flat + 1] = q[:1]
            brow[1, flat : flat + 1] = q[block_x - 1 :]
            bcol[0, flat : flat + 1] = side[2 * groups : 2 * groups + 1]
            bcol[1, flat : flat + 1] = side[2 * groups + 1 : 2 * groups + 2]
            frow[0, flat : flat + 1] = top[f, z, 0]
            frow[1, flat : flat + 1] = bottom[f, z, 0]


def cycle_kernel(groups, fields, block_x, meta, got, piece):
    half = got.shape[1] * 2 // 3
    width = got.shape[2]
    row_block = meta[2 * groups]
    start = meta[2 * row_block]
    rows = got[0, :half]
    sides = None
    for b in range(groups):
        if b:
            rows = rows + got[b, :half]
        lane = iota((width, 2 * width), 0)
        slot = iota((width, 2 * width), 1)
        low = (lane < block_x) & (lane + b * block_x == slot + start) & (slot < PC)
        high = (
            (lane >= block_x)
            & (lane - block_x + b * block_x == slot - width + start)
            & (slot >= width)
            & (slot < width + PC)
        )
        term = jnp.dot(
            got[b, half:], (low | high).astype(F32), precision=HIGH, preferred_element_type=F32
        )
        sides = term if sides is None else sides + term
    piece[:half] = rows
    for z in range(half // (2 * fields)):
        at = half + z * 2 * fields
        piece[at : at + fields] = sides[z * fields : (z + 1) * fields, :width]
        piece[at + fields : at + 2 * fields] = sides[z * fields : (z + 1) * fields, width:]


def level(state, former, coupling, z, first, last, left, right, inverse):
    fields, levels = len(first), state(None, None)
    q = [state(f, z) for f in range(fields)]
    out = []
    for f in range(fields):
        north = jnp.concatenate([q[f][1:], last[f]], axis=0)
        south = jnp.concatenate([first[f], q[f][:-1]], axis=0)
        east = jnp.concatenate([q[f][:, 1:], right[f]], axis=1)
        west = jnp.concatenate([left[f], q[f][:, :-1]], axis=1)
        advect = (q[0] * (north - south) + q[1] * (east - west)) * (0.5 * inverse)
        laplace = (north + south + east + west - 4.0 * q[f]) * (inverse * inverse)
        upper = jnp.where(z < levels - 1, state(f, jnp.minimum(z + 1, levels - 1)), 0.0)
        lower = jnp.where(z > 0, state(f, jnp.maximum(z - 1, 0)), 0.0)
        vertical = 2.0 * q[f] - upper - lower
        coupled = coupling[f, 0] * q[0]
        for g in range(1, fields):
            coupled = coupled + coupling[f, g] * q[g]
        out.append(
            q[f]
            - former(f)
            + time_step * (advect - viscosity * laplace + vertical_mix * vertical + coupled)
        )
    return out


def fold(values):
    total = jnp.sum(values, axis=0, keepdims=True)
    acc = total[:, :128]
    for at in range(128, values.shape[1], 128):
        part = total[:, at : at + 128]
        if part.shape[1] < 128:
            part = jnp.concatenate([part, jnp.zeros((1, 128 - part.shape[1]), F32)], axis=1)
        acc = acc + part
    return acc


def fine_kernel(
    groups, members, meta, coupling, gath, halo, state, old, res, rest, sq, edge, side, fit, thin
):
    z = pl.program_id(0)
    fields, levels = state.shape[:2]
    fine_rows, fine_cols = state.shape[2], state.shape[4]
    piece = fine_rows // RATIO
    block_y = gath.shape[2]
    row_block = meta[2 * groups]
    col_block = meta[2 * groups + 1]
    start_y = meta[2 * row_block + 1]
    half = 2 * fields * levels

    @pl.when(z == 0)
    def _():
        sq[...] = jnp.zeros_like(sq)
        lane = iota((block_y, fine_cols), 0)
        fine = iota((block_y, fine_cols), 1) // RATIO
        rows = None
        cols = gath[0, half:]
        for b in range(members):
            pick = (lane + b * block_y == fine + start_y).astype(F32)
            term = jnp.dot(gath[b, :half], pick, precision=HIGH, preferred_element_type=F32)
            rows = term if rows is None else rows + term
            if b:
                cols = cols + gath[b, half:]
        edge[...] = rows
        pick = iota((128, 128), 0) == piece * col_block + iota((128, 128), 1) // RATIO
        side[...] = jnp.dot(cols, pick.astype(F32), precision=HIGH, preferred_element_type=F32)
        cell = iota((fine_cols, 128), 0) // RATIO + start_y
        fit[...] = (lax.rem(cell, block_y) == iota((fine_cols, 128), 1)).astype(F32).astype(BF16)

    at = pl.multiple_of(z * 2 * fields, 8)
    edges = edge[pl.ds(at, 2 * fields)]
    turned = jnp.transpose(side[pl.ds(at, 2 * fields)])
    first, last, left, right = [], [], [], []
    for f in range(fields):
        above = halo[0, pl.ds(z * fields + f, 1)]
        below = halo[1, pl.ds(z * fields + f, 1)]
        first.append(jnp.where(col_block == 0, edges[f : f + 1], above))
        last.append(jnp.where(col_block == members - 1, edges[fields + f : fields + f + 1], below))
        left.append(turned[:fine_rows, f : f + 1])
        right.append(turned[:fine_rows, fields + f : fields + f + 1])

    def cell(f, at):
        return levels if f is None else state[f, at, :, 0, :]

    got = level(
        cell, lambda f: old[f, 0, :, 0, :], coupling, z, first, last, left, right, float(RATIO)
    )
    squares = None
    for f in range(fields):
        res[f, 0, :, 0, :] = got[f]
        squares = got[f] * got[f] if f == 0 else squares + got[f] * got[f]
        major = got[f].astype(BF16)
        minor = (got[f] - major.astype(F32)).astype(BF16)
        narrow = jnp.dot(major, fit[...], preferred_element_type=F32) + jnp.dot(
            minor, fit[...], preferred_element_type=F32
        )
        thin[f] = narrow * (1.0 / (RATIO * RATIO))
        total = thin[f, pl.ds(0, piece, stride=RATIO), :]
        for k in range(1, RATIO):
            total = total + thin[f, pl.ds(k, piece, stride=RATIO), :]
        rest[f, pl.ds(z, piece, stride=levels), :] = total
    sq[0:1] += fold(squares) * (1.0 / (RATIO * RATIO))


def base_kernel(groups, members, meta, coupling, rows, cols, state, old, res, sq):
    z = pl.program_id(0)
    fields, levels, block_x, block_y = state.shape
    row_block = meta[2 * groups]
    col_block = meta[2 * groups + 1]

    @pl.when(z == 0)
    def _():
        sq[...] = jnp.zeros_like(sq)

    first, last, left, right = [], [], [], []
    for f in range(fields):
        at = z * fields + f
        first.append(jnp.where(row_block > 0, rows[0, pl.ds(at, 1)], 0.0))
        last.append(jnp.where(row_block < groups - 1, rows[1, pl.ds(at, 1)], 0.0))
        left.append(jnp.where(col_block > 0, cols[0, pl.ds(at, 1)], 0.0))
        right.append(jnp.where(col_block < members - 1, cols[1, pl.ds(at, 1)], 0.0))
    turned = jnp.transpose(jnp.concatenate(left + right, axis=0))
    left = [turned[:, f : f + 1] for f in range(fields)]
    right = [turned[:, fields + f : fields + f + 1] for f in range(fields)]

    def cell(f, at):
        return levels if f is None else state[f, at]

    got = level(cell, lambda f: old[f, 0], coupling, z, first, last, left, right, 1.0)
    x = iota((block_x, block_y), 0) + row_block * block_x
    y = iota((block_x, block_y), 1) + col_block * block_y
    covered = jnp.zeros((block_x, block_y), jnp.bool_)
    for g in range(groups):
        dx, dy = x - meta[2 * g], y - meta[2 * g + 1]
        covered = covered | ((dx >= 0) & (dx < PC) & (dy >= 0) & (dy < PC))
    squares = None
    for f in range(fields):
        res[f, 0] = got[f]
        squares = got[f] * got[f] if f == 0 else squares + got[f] * got[f]
    sq[0:1] += fold(jnp.where(covered, 0.0, squares))


def sort_kernel(groups, members, block_x, meta, got, sums, slots, total):
    fields, depth, block_y = got.shape[1:]
    levels = depth * RATIO // (PC * RATIO // members)
    piece = depth // levels
    row_block = meta[2 * groups]
    col_block = meta[2 * groups + 1]
    acc = sums[0]
    for g in range(1, groups):
        acc = acc + sums[g]
    total[...] = acc
    for g in range(groups):
        begin = meta[2 * g] + col_block * piece - row_block * block_x
        start_y = meta[2 * g + 1]
        here = (begin < block_x) & (begin + piece > 0)
        for b in range(members):
            shift = start_y - b * block_y

            @pl.when(here & (shift < block_y) & (shift + PC > 0))
            def _():
                lane = iota((depth, block_y), 1)
                inside = (lane >= shift) & (lane < shift + PC)
                for f in range(fields):
                    slots[b, f] = jnp.where(inside, got[g, f], slots[b, f])


def place_kernel(groups, members, meta, tend, got, sums, out, norm, laid):
    fields, levels, block_x, block_y = tend.shape
    depth = got.shape[2]
    piece = depth // levels
    row_block = meta[2 * groups]
    col_block = meta[2 * groups + 1]
    acc = sums[0]
    for b in range(1, members):
        acc = acc + sums[b]
    norm[...] = jnp.sqrt(jnp.sum(acc, keepdims=True))
    x = iota((block_x, block_y), 0) + row_block * block_x
    y = iota((block_x, block_y), 1) + col_block * block_y
    covered = jnp.zeros((block_x, block_y), jnp.bool_)
    for g in range(groups):
        dx, dy = x - meta[2 * g], y - meta[2 * g + 1]
        covered = covered | ((dx >= 0) & (dx < PC) & (dy >= 0) & (dy < PC))
        begin = meta[2 * g] - row_block * block_x
        shift = meta[2 * g + 1] - col_block * block_y

        @pl.when((begin < block_x) & (begin + PC > 0) & (shift < block_y) & (shift + PC > 0))
        def _():
            lane = iota((levels, block_y), 1)
            inside = (lane >= shift) & (lane < shift + PC)

            def row(at, carry):
                patch_row = at - begin
                part = patch_row // piece
                source = pl.multiple_of((patch_row - part * piece) * levels, levels)
                target = pl.multiple_of(at * levels, levels)
                for f in range(fields):
                    laid[f, pl.ds(target, levels)] = jnp.where(
                        inside,
                        got[part, f, pl.ds(source, levels)],
                        laid[f, pl.ds(target, levels)],
                    )
                return carry

            lax.fori_loop(jnp.maximum(begin, 0), jnp.minimum(begin + PC, block_x), row, 0)

    for f in range(fields):
        for z in range(levels):
            out[f, z] = jnp.where(
                covered, laid[f, pl.ds(z, block_x, stride=levels), :], tend[f, z]
            )


def local(sizes, base_state, base_old, fine_state, fine_old, coupling, patch_offsets, patch_group):
    groups, members = sizes["gx"], sizes["gy"]
    fields, levels, block_x, block_y = base_state.shape
    fine_rows, fine_cols = fine_state.shape[3:]
    piece = fine_rows // RATIO
    flat = fields * levels
    def shape(*dims):
        return jax.ShapeDtypeStruct(dims, F32)

    tail = fine_rows - 1
    fine_turned = jnp.swapaxes(fine_state, 2, 3)
    cyc, brow, bcol, frow, meta = pl.pallas_call(
        functools.partial(prepare_kernel, groups),
        grid=(1,),
        out_shape=[
            shape(groups, 3 * flat, block_y),
            shape(2, flat, block_y),
            shape(2, flat, block_x),
            shape(2, flat, fine_cols),
            jax.ShapeDtypeStruct((2 * groups + 2,), jnp.int32),
        ],
        in_specs=[
            SMEM,
            SMEM,
            VMEM,
            pl.BlockSpec((fields, levels, 1, 1, fine_cols), lambda i: (0, 0, 0, 0, 0)),
            pl.BlockSpec((fields, levels, 1, 1, fine_cols), lambda i: (0, 0, tail, 0, 0)),
        ],
        out_specs=[VMEM] * 4 + [SMEM],
        compiler_params=params(),
        name="prepare",
    )(patch_offsets, patch_group, base_state, fine_turned, fine_turned)

    cyc, brow, bcol, frow = communicate(
        "edges",
        1,
        sizes,
        (("exchange", "gx"), ("shift", "gx"), ("shift", "gy"), ("shift", "gy")),
        cyc,
        brow,
        bcol,
        frow,
    )
    cycle = pl.pallas_call(
        functools.partial(cycle_kernel, groups, fields, block_x),
        out_shape=shape(4 * flat, block_y),
        in_specs=[SMEM, VMEM],
        out_specs=VMEM,
        compiler_params=params(),
        name="cycle",
    )(meta, cyc)
    (gath,) = communicate("members", 2, sizes, (("gather", "gy"),), cycle)

    slab = (fields, levels, fine_rows, 1, fine_cols)
    thin = (fields, 1, fine_rows, 1, fine_cols)
    fine_res, rest, fine_sq = pl.pallas_call(
        functools.partial(fine_kernel, groups, members),
        grid=(levels,),
        out_shape=[shape(*slab), shape(fields, piece * levels, 128), shape(8, 128)],
        in_specs=[
            SMEM,
            SMEM,
            VMEM,
            VMEM,
            pl.BlockSpec(slab, lambda z: (0, 0, 0, 0, 0)),
            pl.BlockSpec(thin, lambda z: (0, z, 0, 0, 0)),
        ],
        out_specs=[
            pl.BlockSpec(thin, lambda z: (0, z, 0, 0, 0)),
            pl.BlockSpec((fields, piece * levels, 128), lambda z: (0, 0, 0)),
            pl.BlockSpec((8, 128), lambda z: (0, 0)),
        ],
        scratch_shapes=[
            pltpu.VMEM((2 * flat, fine_cols), F32),
            pltpu.VMEM((2 * flat, 128), F32),
            pltpu.VMEM((fine_cols, 128), BF16),
            pltpu.VMEM((fields, fine_rows, 128), F32),
        ],
        compiler_params=params(),
        name="fine",
    )(meta, coupling, gath, frow, fine_turned, jnp.swapaxes(fine_old, 2, 3))

    whole = (fields, levels, block_x, block_y)
    sheet = (fields, 1, block_x, block_y)
    tend, base_sq = pl.pallas_call(
        functools.partial(base_kernel, groups, members),
        grid=(levels,),
        out_shape=[shape(*whole), shape(8, 128)],
        in_specs=[
            SMEM,
            SMEM,
            VMEM,
            VMEM,
            pl.BlockSpec(whole, lambda z: (0, 0, 0, 0)),
            pl.BlockSpec(sheet, lambda z: (0, z, 0, 0)),
        ],
        out_specs=[
            pl.BlockSpec(sheet, lambda z: (0, z, 0, 0)),
            pl.BlockSpec((8, 128), lambda z: (0, 0)),
        ],
        compiler_params=params(),
        name="base",
    )(meta, coupling, brow, bcol, base_state, base_old)

    gathered, sums = communicate(
        "owners", 3, sizes, (("relay", "gx"), ("gather", "gx")), rest, fine_sq + base_sq
    )
    slots, total = pl.pallas_call(
        functools.partial(sort_kernel, groups, members, block_x),
        out_shape=[shape(members, fields, piece * levels, block_y), shape(8, 128)],
        in_specs=[SMEM, VMEM, VMEM],
        out_specs=[VMEM, VMEM],
        compiler_params=params(),
        name="sort",
    )(meta, gathered, sums)
    slots, sums = communicate(
        "columns", 4, sizes, (("exchange", "gy"), ("gather", "gy")), slots, total
    )
    base_out, norm = pl.pallas_call(
        functools.partial(place_kernel, groups, members),
        out_shape=[shape(*whole), shape(1, 1)],
        in_specs=[SMEM, VMEM, VMEM, VMEM],
        out_specs=[VMEM, VMEM],
        scratch_shapes=[pltpu.VMEM((fields, block_x * levels, block_y), F32)],
        compiler_params=params(),
        name="place",
    )(meta, tend, slots, sums)
    return (base_out, jnp.swapaxes(fine_res, 2, 3), norm[0, 0])


def solution(mesh):
    placed = (
        P(None, None, "gx", "gy"),
        P(None, None, "gx", "gy"),
        P(None, None, "gx", "gy", None),
        P(None, None, "gx", "gy", None),
        P(),
        P(),
        P(),
    )
    return jax.shard_map(
        functools.partial(local, dict(mesh.shape)),
        mesh=mesh,
        in_specs=placed,
        out_specs=(P(None, None, "gx", "gy"), P(None, None, "gx", "gy", None), P()),
        check_vma=False,
    )
```

```python
import functools

import jax
import jax.numpy as jnp
from jax import lax
from jax.experimental import pallas as pl
from jax.experimental.pallas import tpu as pltpu
from jax.sharding import PartitionSpec as P

PC = 88
RATIO = 3

time_step = 0.1
viscosity = 0.2
vertical_mix = 0.5

F32 = jnp.float32
BF16 = jnp.bfloat16
HIGH = lax.Precision.HIGHEST
MESH = pl.DeviceIdType.MESH
VMEM = pl.BlockSpec(memory_space=pltpu.VMEM)
SMEM = pl.BlockSpec(memory_space=pltpu.SMEM)


def params(**more):
    return pltpu.CompilerParams(vmem_limit_bytes=58 * 1024 * 1024, **more)


def iota(shape, dim):
    return lax.broadcasted_iota(jnp.int32, shape, dim)


def comm_kernel(plan, axes, inner, *refs):
    count = len(plan)
    sources, targets = refs[:count], refs[count : 2 * count]
    send_sem, recv_sem, local_sem = refs[2 * count :]
    barrier = pltpu.get_barrier_semaphore()
    total = 0
    for axis, size in axes.items():
        me = lax.axis_index(axis)
        for step in range(1, size):
            pl.semaphore_signal(
                barrier, inc=1, device_id={axis: lax.rem(me + step, size)}, device_id_type=MESH
            )
        total += size - 1
    pl.semaphore_wait(barrier, total)
    used = [0]
    waiting = []

    def send(source, target, axis, peer):
        slot = used[0]
        used[0] += 1
        copy = pltpu.make_async_remote_copy(
            src_ref=source,
            dst_ref=target,
            send_sem=send_sem.at[slot],
            recv_sem=recv_sem.at[slot],
            device_id={axis: peer},
            device_id_type=MESH,
        )
        copy.start()
        return copy

    relays = []
    local = []
    for index, (mode, axis) in enumerate(plan):
        source, target = sources[index], targets[index]
        size = axes[axis]
        me = lax.axis_index(axis)
        if mode == "shift":
            up, down = lax.rem(me + 1, size), lax.rem(me + size - 1, size)
            waiting.append(send(source.at[1], target.at[0], axis, up))
            waiting.append(send(source.at[0], target.at[1], axis, down))
            continue
        own = pltpu.make_async_copy(
            source.at[me] if mode == "exchange" else source, target.at[me], local_sem.at[index]
        )
        own.start()
        local.append(own)
        if mode == "relay":
            relays.append((source, target, axis))
            continue
        for step in range(1, size):
            peer = lax.rem(me + step, size)
            part = source.at[peer] if mode == "exchange" else source
            waiting.append(send(part, target.at[me], axis, peer))
    for source, target, axis in relays:
        relay(source, target, axis, axes[axis], inner, send_sem, recv_sem, used[0])
    for copy in waiting:
        copy.wait()
    for copy in local:
        copy.wait()


def communicate(name, ident, sizes, plan, *arrays):
    axes = {axis: sizes[axis] for _, axis in plan}
    inner = 1
    while (2 * inner) ** 2 <= sizes["gx"]:
        inner *= 2
    slots = 0
    shapes = []
    for (mode, axis), array in zip(plan, arrays):
        size = axes[axis]
        if mode == "shift":
            slots += 2
            shapes.append(array.shape)
        elif mode == "exchange":
            slots += size - 1
            shapes.append(array.shape)
        else:
            slots += len(relay_slots(array.shape[0], size, inner)) if mode == "relay" else size - 1
            shapes.append((size, *array.shape))
    return pl.pallas_call(
        functools.partial(comm_kernel, plan, axes, inner),
        out_shape=[jax.ShapeDtypeStruct(s, F32) for s in shapes],
        in_specs=[VMEM] * len(plan),
        out_specs=[VMEM] * len(plan),
        scratch_shapes=[
            pltpu.SemaphoreType.DMA((slots,)),
            pltpu.SemaphoreType.DMA((slots,)),
            pltpu.SemaphoreType.DMA((len(plan),)),
        ],
        compiler_params=params(collective_id=ident, has_side_effects=True),
        name=name,
    )(*arrays)


def relay_slots(fields, size, inner):
    outer = size // inner
    keys = [("own", f, 0, hop) for f in range(fields) for hop in range(1, inner)]
    for f in range(fields):
        if f < fields // 2:
            for way in ("up", "down"):
                keys += [(way, f, 0, d) for d in range(1, outer)]
                keys += [
                    (way + "x", f, hop, d) for d in range(1, outer) for hop in range(1, inner)
                ]
        else:
            for way in ("up", "down"):
                keys += [(way, f, hop, d) for d in range(1, outer) for hop in range(inner)]
    return {key: slot for slot, key in enumerate(keys)}


def relay(source, target, axis, size, inner, send_sem, recv_sem, base):
    fields = source.shape[0]
    outer = size // inner
    me = lax.axis_index(axis)
    high, low = lax.div(me, inner), lax.rem(me, inner)
    slots = relay_slots(fields, size, inner)
    has_up, has_down = high < outer - 1, high > 0
    early, late = range(fields // 2), range(fields // 2, fields)

    def place(step, hop):
        return (high - step) * inner + lax.rem(low + inner - hop, inner)

    def across(hop):
        return high * inner + lax.rem(low + hop, inner)

    def copy(key, origin, peer, own=False):
        return pltpu.make_async_remote_copy(
            src_ref=source.at[key[1]] if own else target.at[origin, key[1]],
            dst_ref=target.at[origin, key[1]],
            send_sem=send_sem.at[base + slots[key]],
            recv_sem=recv_sem.at[base + slots[key]],
            device_id={axis: peer},
            device_id_type=MESH,
        )

    finish = []

    def start(key, origin, peer, own, *conditions):
        ready = conditions[0] if conditions else None
        for more in conditions[1:]:
            ready = ready & more
        made = copy(key, origin, peer, own)
        if ready is None:
            made.start()
        else:
            pl.when(ready)(made.start)
        finish.append((made, ready))

    for f in (*late, *early):
        for hop in range(1, inner):
            start(("own", f, 0, hop), me, across(hop), True)
        start(("up", f, 0, 1), me, me + inner, True, has_up)
        start(("down", f, 0, 1), me, me - inner, True, has_down)
    for f in late:
        for hop in range(1, inner):
            origin = place(0, hop)
            copy(("own", f, 0, hop), origin, me).wait_recv()
            start(("up", f, hop, 1), origin, me + inner, False, has_up)
            start(("down", f, hop, 1), origin, me - inner, False, has_down)
    for d in range(1, outer):
        for f in range(fields):
            for hop in range(1 if f in early else inner):
                for way, sign, exists, onward in (
                    ("up", 1, high >= d, has_up),
                    ("down", -1, high + d < outer, has_down),
                ):
                    origin = place(sign * d, hop)
                    pl.when(exists)(copy((way, f, hop, d), origin, me).wait_recv)
                    if d + 1 < outer:
                        start(
                            (way, f, hop, d + 1), origin, me + sign * inner, False, exists, onward
                        )
                    if f in early:
                        for jump in range(1, inner):
                            start((way + "x", f, jump, d), origin, across(jump), False, exists)
    for f in early:
        for hop in range(1, inner):
            copy(("own", f, 0, hop), place(0, hop), me).wait_recv()
            for d in range(1, outer):
                got = copy(("upx", f, hop, d), place(d, hop), me)
                pl.when(high >= d)(got.wait_recv)
                got = copy(("downx", f, hop, d), place(-d, hop), me)
                pl.when(high + d < outer)(got.wait_recv)
    for made, ready in finish:
        if ready is None:
            made.wait_send()
        else:
            pl.when(ready)(made.wait_send)


def prepare_kernel(groups, offsets, owners, base, top, bottom, cyc, brow, bcol, frow, meta):
    fields, levels, block_x, block_y = base.shape
    row_block = lax.axis_index("gx")
    col_block = lax.axis_index("gy")
    meta[2 * groups] = row_block
    meta[2 * groups + 1] = col_block
    row_pick = jnp.full((2 * groups, block_x), -1, jnp.int32)
    col_pick = jnp.full((2 * groups + 8, block_y), -1, jnp.int32)
    row_slot = iota(row_pick.shape, 0)
    col_slot = iota(col_pick.shape, 0)
    for p in range(groups):
        g = owners[p]
        meta[2 * g] = offsets[p, 0]
        meta[2 * g + 1] = offsets[p, 1]
        row = offsets[p, 0] - row_block * block_x
        col = offsets[p, 1] - col_block * block_y
        row_pick = jnp.where(row_slot == g, row - 1, row_pick)
        row_pick = jnp.where(row_slot == g + groups, row + PC, row_pick)
        col_pick = jnp.where(col_slot == g, col - 1, col_pick)
        col_pick = jnp.where(col_slot == g + groups, col + PC, col_pick)
    col_pick = jnp.where(col_slot == 2 * groups, 0, col_pick)
    col_pick = jnp.where(col_slot == 2 * groups + 1, block_y - 1, col_pick)
    pick_rows = (iota(row_pick.shape, 1) == row_pick).astype(F32)
    pick_cols = (iota(col_pick.shape, 1) == col_pick).astype(F32)
    for z in range(levels):
        for f in range(fields):
            q = base[f, z]
            flat = z * fields + f
            found = jnp.dot(pick_rows, q, precision=HIGH, preferred_element_type=F32)
            side = lax.dot_general(
                pick_cols, q, (((1,), (1,)), ((), ())), precision=HIGH, preferred_element_type=F32
            )
            both = jnp.concatenate([side[:groups], side[groups : 2 * groups]], axis=1)
            for g in range(groups):
                high = z * 2 * fields + f
                cyc[g, high : high + 1] = found[g : g + 1]
                cyc[g, high + fields : high + fields + 1] = found[groups + g : groups + g + 1]
                at = 2 * fields * levels + flat
                cyc[g, at : at + 1] = both[g : g + 1]
            brow[0, flat : flat + 1] = q[:1]
            brow[1, flat : flat + 1] = q[block_x - 1 :]
            bcol[0, flat : flat + 1] = side[2 * groups : 2 * groups + 1]
            bcol[1, flat : flat + 1] = side[2 * groups + 1 : 2 * groups + 2]
            frow[0, flat : flat + 1] = top[f, z, 0]
            frow[1, flat : flat + 1] = bottom[f, z, 0]


def cycle_kernel(groups, fields, block_x, meta, got, piece):
    half = got.shape[1] * 2 // 3
    width = got.shape[2]
    row_block = meta[2 * groups]
    start = meta[2 * row_block]
    rows = got[0, :half]
    sides = None
    for b in range(groups):
        if b:
            rows = rows + got[b, :half]
        lane = iota((width, 2 * width), 0)
        slot = iota((width, 2 * width), 1)
        low = (lane < block_x) & (lane + b * block_x == slot + start) & (slot < PC)
        high = (
            (lane >= block_x)
            & (lane - block_x + b * block_x == slot - width + start)
            & (slot >= width)
            & (slot < width + PC)
        )
        term = jnp.dot(
            got[b, half:], (low | high).astype(F32), precision=HIGH, preferred_element_type=F32
        )
        sides = term if sides is None else sides + term
    piece[:half] = rows
    for z in range(half // (2 * fields)):
        at = half + z * 2 * fields
        piece[at : at + fields] = sides[z * fields : (z + 1) * fields, :width]
        piece[at + fields : at + 2 * fields] = sides[z * fields : (z + 1) * fields, width:]


def level(state, former, coupling, z, first, last, left, right, inverse):
    fields, levels = len(first), state(None, None)
    q = [state(f, z) for f in range(fields)]
    out = []
    for f in range(fields):
        north = jnp.concatenate([q[f][1:], last[f]], axis=0)
        south = jnp.concatenate([first[f], q[f][:-1]], axis=0)
        east = jnp.concatenate([q[f][:, 1:], right[f]], axis=1)
        west = jnp.concatenate([left[f], q[f][:, :-1]], axis=1)
        advect = (q[0] * (north - south) + q[1] * (east - west)) * (0.5 * inverse)
        laplace = (north + south + east + west - 4.0 * q[f]) * (inverse * inverse)
        upper = jnp.where(z < levels - 1, state(f, jnp.minimum(z + 1, levels - 1)), 0.0)
        lower = jnp.where(z > 0, state(f, jnp.maximum(z - 1, 0)), 0.0)
        vertical = 2.0 * q[f] - upper - lower
        coupled = coupling[f, 0] * q[0]
        for g in range(1, fields):
            coupled = coupled + coupling[f, g] * q[g]
        out.append(
            q[f]
            - former(f)
            + time_step * (advect - viscosity * laplace + vertical_mix * vertical + coupled)
        )
    return out


def fold(values):
    total = jnp.sum(values, axis=0, keepdims=True)
    acc = total[:, :128]
    for at in range(128, values.shape[1], 128):
        part = total[:, at : at + 128]
        if part.shape[1] < 128:
            part = jnp.concatenate([part, jnp.zeros((1, 128 - part.shape[1]), F32)], axis=1)
        acc = acc + part
    return acc


def fine_kernel(
    groups, members, meta, coupling, gath, halo, state, old, res, rest, sq, edge, side, fit, thin, ring
):
    z = pl.program_id(0)
    fields, levels = state.shape[:2]
    fine_rows, fine_cols = state.shape[2], state.shape[4]
    piece = fine_rows // RATIO
    block_y = gath.shape[2]
    row_block = meta[2 * groups]
    col_block = meta[2 * groups + 1]
    start_y = meta[2 * row_block + 1]
    half = 2 * fields * levels

    @pl.when(z == 0)
    def _():
        sq[...] = jnp.zeros_like(sq)
        lane = iota((block_y, fine_cols), 0)
        fine = iota((block_y, fine_cols), 1) // RATIO
        rows = None
        cols = gath[0, half:]
        for b in range(members):
            pick = (lane + b * block_y == fine + start_y).astype(F32)
            term = jnp.dot(gath[b, :half], pick, precision=HIGH, preferred_element_type=F32)
            rows = term if rows is None else rows + term
            if b:
                cols = cols + gath[b, half:]
        edge[...] = rows
        pick = iota((128, 128), 0) == piece * col_block + iota((128, 128), 1) // RATIO
        side[...] = jnp.dot(cols, pick.astype(F32), precision=HIGH, preferred_element_type=F32)
        cell = iota((fine_cols, 128), 0) // RATIO + start_y
        fit[...] = (lax.rem(cell, block_y) == iota((fine_cols, 128), 1)).astype(F32).astype(BF16)

        for f in range(fields):
            ring[0, f] = state[f, 0, :, 0, :]

    @pl.when(z + 1 < levels)
    def _():
        for f in range(fields):
            ring[lax.rem(z + 1, 3), f] = state[f, z + 1, :, 0, :]

    at = pl.multiple_of(z * 2 * fields, 8)
    edges = edge[pl.ds(at, 2 * fields)]
    turned = jnp.transpose(side[pl.ds(at, 2 * fields)])
    first, last, left, right = [], [], [], []
    for f in range(fields):
        above = halo[0, pl.ds(z * fields + f, 1)]
        below = halo[1, pl.ds(z * fields + f, 1)]
        first.append(jnp.where(col_block == 0, edges[f : f + 1], above))
        last.append(jnp.where(col_block == members - 1, edges[fields + f : fields + f + 1], below))
        left.append(turned[:fine_rows, f : f + 1])
        right.append(turned[:fine_rows, fields + f : fields + f + 1])

    def cell(f, at):
        return levels if f is None else ring[lax.rem(at, 3), f]

    got = level(
        cell, lambda f: old[f, 0, :, 0, :], coupling, z, first, last, left, right, float(RATIO)
    )
    squares = None
    for f in range(fields):
        res[f, 0, :, 0, :] = got[f]
        squares = got[f] * got[f] if f == 0 else squares + got[f] * got[f]
        major = got[f].astype(BF16)
        minor = (got[f] - major.astype(F32)).astype(BF16)
        narrow = jnp.dot(major, fit[...], preferred_element_type=F32) + jnp.dot(
            minor, fit[...], preferred_element_type=F32
        )
        thin[f] = narrow * (1.0 / (RATIO * RATIO))
        total = thin[f, pl.ds(0, piece, stride=RATIO), :]
        for k in range(1, RATIO):
            total = total + thin[f, pl.ds(k, piece, stride=RATIO), :]
        rest[f, pl.ds(z, piece, stride=levels), :] = total
    sq[0:1] += fold(squares) * (1.0 / (RATIO * RATIO))


def base_kernel(groups, members, meta, coupling, rows, cols, state, old, res, sq):
    z = pl.program_id(0)
    fields, levels, block_x, block_y = state.shape
    row_block = meta[2 * groups]
    col_block = meta[2 * groups + 1]

    @pl.when(z == 0)
    def _():
        sq[...] = jnp.zeros_like(sq)

    first, last, left, right = [], [], [], []
    for f in range(fields):
        at = z * fields + f
        first.append(jnp.where(row_block > 0, rows[0, pl.ds(at, 1)], 0.0))
        last.append(jnp.where(row_block < groups - 1, rows[1, pl.ds(at, 1)], 0.0))
        left.append(jnp.where(col_block > 0, cols[0, pl.ds(at, 1)], 0.0))
        right.append(jnp.where(col_block < members - 1, cols[1, pl.ds(at, 1)], 0.0))
    turned = jnp.transpose(jnp.concatenate(left + right, axis=0))
    left = [turned[:, f : f + 1] for f in range(fields)]
    right = [turned[:, fields + f : fields + f + 1] for f in range(fields)]

    def cell(f, at):
        return levels if f is None else state[f, at]

    got = level(cell, lambda f: old[f, 0], coupling, z, first, last, left, right, 1.0)
    x = iota((block_x, block_y), 0) + row_block * block_x
    y = iota((block_x, block_y), 1) + col_block * block_y
    covered = jnp.zeros((block_x, block_y), jnp.bool_)
    for g in range(groups):
        dx, dy = x - meta[2 * g], y - meta[2 * g + 1]
        covered = covered | ((dx >= 0) & (dx < PC) & (dy >= 0) & (dy < PC))
    squares = None
    for f in range(fields):
        res[f, 0] = got[f]
        squares = got[f] * got[f] if f == 0 else squares + got[f] * got[f]
    sq[0:1] += fold(jnp.where(covered, 0.0, squares))


def sort_kernel(groups, members, block_x, meta, got, sums, slots, total):
    fields, depth, block_y = got.shape[1:]
    levels = depth * RATIO // (PC * RATIO // members)
    piece = depth // levels
    row_block = meta[2 * groups]
    col_block = meta[2 * groups + 1]
    acc = sums[0]
    for g in range(1, groups):
        acc = acc + sums[g]
    total[...] = acc
    for g in range(groups):
        begin = meta[2 * g] + col_block * piece - row_block * block_x
        start_y = meta[2 * g + 1]
        here = (begin < block_x) & (begin + piece > 0)
        for b in range(members):
            shift = start_y - b * block_y

            @pl.when(here & (shift < block_y) & (shift + PC > 0))
            def _():
                lane = iota((depth, block_y), 1)
                inside = (lane >= shift) & (lane < shift + PC)
                for f in range(fields):
                    slots[b, f] = jnp.where(inside, got[g, f], slots[b, f])


def place_kernel(groups, members, meta, tend, got, sums, out, norm, laid):
    fields, levels, block_x, block_y = tend.shape
    depth = got.shape[2]
    piece = depth // levels
    row_block = meta[2 * groups]
    col_block = meta[2 * groups + 1]
    acc = sums[0]
    for b in range(1, members):
        acc = acc + sums[b]
    norm[...] = jnp.sqrt(jnp.sum(acc, keepdims=True))
    x = iota((block_x, block_y), 0) + row_block * block_x
    y = iota((block_x, block_y), 1) + col_block * block_y
    covered = jnp.zeros((block_x, block_y), jnp.bool_)
    for g in range(groups):
        dx, dy = x - meta[2 * g], y - meta[2 * g + 1]
        covered = covered | ((dx >= 0) & (dx < PC) & (dy >= 0) & (dy < PC))
        begin = meta[2 * g] - row_block * block_x
        shift = meta[2 * g + 1] - col_block * block_y

        @pl.when((begin < block_x) & (begin + PC > 0) & (shift < block_y) & (shift + PC > 0))
        def _():
            lane = iota((levels, block_y), 1)
            inside = (lane >= shift) & (lane < shift + PC)

            def row(at, carry):
                patch_row = at - begin
                part = patch_row // piece
                source = pl.multiple_of((patch_row - part * piece) * levels, levels)
                target = pl.multiple_of(at * levels, levels)
                for f in range(fields):
                    laid[f, pl.ds(target, levels)] = jnp.where(
                        inside,
                        got[part, f, pl.ds(source, levels)],
                        laid[f, pl.ds(target, levels)],
                    )
                return carry

            lax.fori_loop(jnp.maximum(begin, 0), jnp.minimum(begin + PC, block_x), row, 0)

    for f in range(fields):
        for z in range(levels):
            out[f, z] = jnp.where(
                covered, laid[f, pl.ds(z, block_x, stride=levels), :], tend[f, z]
            )


def local(sizes, base_state, base_old, fine_state, fine_old, coupling, patch_offsets, patch_group):
    groups, members = sizes["gx"], sizes["gy"]
    fields, levels, block_x, block_y = base_state.shape
    fine_rows, fine_cols = fine_state.shape[3:]
    piece = fine_rows // RATIO
    flat = fields * levels
    def shape(*dims):
        return jax.ShapeDtypeStruct(dims, F32)

    tail = fine_rows - 1
    fine_turned = jnp.swapaxes(fine_state, 2, 3)
    cyc, brow, bcol, frow, meta = pl.pallas_call(
        functools.partial(prepare_kernel, groups),
        grid=(1,),
        out_shape=[
            shape(groups, 3 * flat, block_y),
            shape(2, flat, block_y),
            shape(2, flat, block_x),
            shape(2, flat, fine_cols),
            jax.ShapeDtypeStruct((2 * groups + 2,), jnp.int32),
        ],
        in_specs=[
            SMEM,
            SMEM,
            VMEM,
            pl.BlockSpec((fields, levels, 1, 1, fine_cols), lambda i: (0, 0, 0, 0, 0)),
            pl.BlockSpec((fields, levels, 1, 1, fine_cols), lambda i: (0, 0, tail, 0, 0)),
        ],
        out_specs=[VMEM] * 4 + [SMEM],
        compiler_params=params(),
        name="prepare",
    )(patch_offsets, patch_group, base_state, fine_turned, fine_turned)

    cyc, brow, bcol, frow = communicate(
        "edges",
        1,
        sizes,
        (("exchange", "gx"), ("shift", "gx"), ("shift", "gy"), ("shift", "gy")),
        cyc,
        brow,
        bcol,
        frow,
    )
    cycle = pl.pallas_call(
        functools.partial(cycle_kernel, groups, fields, block_x),
        out_shape=shape(4 * flat, block_y),
        in_specs=[SMEM, VMEM],
        out_specs=VMEM,
        compiler_params=params(),
        name="cycle",
    )(meta, cyc)
    (gath,) = communicate("members", 2, sizes, (("gather", "gy"),), cycle)

    slab = (fields, levels, fine_rows, 1, fine_cols)
    thin = (fields, 1, fine_rows, 1, fine_cols)
    fine_res, rest, fine_sq = pl.pallas_call(
        functools.partial(fine_kernel, groups, members),
        grid=(levels,),
        out_shape=[shape(*slab), shape(fields, piece * levels, 128), shape(8, 128)],
        in_specs=[
            SMEM,
            SMEM,
            VMEM,
            VMEM,
            pl.BlockSpec(slab, lambda z: (0, 0, 0, 0, 0)),
            pl.BlockSpec(thin, lambda z: (0, z, 0, 0, 0)),
        ],
        out_specs=[
            pl.BlockSpec(thin, lambda z: (0, z, 0, 0, 0)),
            pl.BlockSpec((fields, piece * levels, 128), lambda z: (0, 0, 0)),
            pl.BlockSpec((8, 128), lambda z: (0, 0)),
        ],
        scratch_shapes=[
            pltpu.VMEM((2 * flat, fine_cols), F32),
            pltpu.VMEM((2 * flat, 128), F32),
            pltpu.VMEM((fine_cols, 128), BF16),
            pltpu.VMEM((fields, fine_rows, 128), F32),
            pltpu.VMEM((3, fields, fine_rows, fine_cols), F32),
        ],
        compiler_params=params(),
        name="fine",
    )(meta, coupling, gath, frow, fine_turned, jnp.swapaxes(fine_old, 2, 3))

    whole = (fields, levels, block_x, block_y)
    sheet = (fields, 1, block_x, block_y)
    tend, base_sq = pl.pallas_call(
        functools.partial(base_kernel, groups, members),
        grid=(levels,),
        out_shape=[shape(*whole), shape(8, 128)],
        in_specs=[
            SMEM,
            SMEM,
            VMEM,
            VMEM,
            pl.BlockSpec(whole, lambda z: (0, 0, 0, 0)),
            pl.BlockSpec(sheet, lambda z: (0, z, 0, 0)),
        ],
        out_specs=[
            pl.BlockSpec(sheet, lambda z: (0, z, 0, 0)),
            pl.BlockSpec((8, 128), lambda z: (0, 0)),
        ],
        compiler_params=params(),
        name="base",
    )(meta, coupling, brow, bcol, base_state, base_old)

    gathered, sums = communicate(
        "owners", 3, sizes, (("relay", "gx"), ("gather", "gx")), rest, fine_sq + base_sq
    )
    slots, total = pl.pallas_call(
        functools.partial(sort_kernel, groups, members, block_x),
        out_shape=[shape(members, fields, piece * levels, block_y), shape(8, 128)],
        in_specs=[SMEM, VMEM, VMEM],
        out_specs=[VMEM, VMEM],
        compiler_params=params(),
        name="sort",
    )(meta, gathered, sums)
    slots, sums = communicate(
        "columns", 4, sizes, (("exchange", "gy"), ("gather", "gy")), slots, total
    )
    base_out, norm = pl.pallas_call(
        functools.partial(place_kernel, groups, members),
        out_shape=[shape(*whole), shape(1, 1)],
        in_specs=[SMEM, VMEM, VMEM, VMEM],
        out_specs=[VMEM, VMEM],
        scratch_shapes=[pltpu.VMEM((fields, block_x * levels, block_y), F32)],
        compiler_params=params(),
        name="place",
    )(meta, tend, slots, sums)
    return (base_out, jnp.swapaxes(fine_res, 2, 3), norm[0, 0])


def solution(mesh):
    placed = (
        P(None, None, "gx", "gy"),
        P(None, None, "gx", "gy"),
        P(None, None, "gx", "gy", None),
        P(None, None, "gx", "gy", None),
        P(),
        P(),
        P(),
    )
    return jax.shard_map(
        functools.partial(local, dict(mesh.shape)),
        mesh=mesh,
        in_specs=placed,
        out_specs=(P(None, None, "gx", "gy"), P(None, None, "gx", "gy", None), P()),
        check_vma=False,
    )
```

```python
import functools

import jax
import jax.numpy as jnp
from jax import lax
from jax.experimental import pallas as pl
from jax.experimental.pallas import tpu as pltpu
from jax.sharding import PartitionSpec as P

PC = 88
RATIO = 3

time_step = 0.1
viscosity = 0.2
vertical_mix = 0.5

F32 = jnp.float32
BF16 = jnp.bfloat16
HIGH = lax.Precision.HIGHEST
MESH = pl.DeviceIdType.MESH
VMEM = pl.BlockSpec(memory_space=pltpu.VMEM)
SMEM = pl.BlockSpec(memory_space=pltpu.SMEM)


def params(**more):
    return pltpu.CompilerParams(vmem_limit_bytes=58 * 1024 * 1024, **more)


def iota(shape, dim):
    return lax.broadcasted_iota(jnp.int32, shape, dim)


def comm_kernel(plan, axes, inner, *refs):
    count = len(plan)
    sources, targets = refs[:count], refs[count : 2 * count]
    send_sem, recv_sem, local_sem = refs[2 * count :]
    barrier = pltpu.get_barrier_semaphore()
    total = 0
    for axis, size in axes.items():
        me = lax.axis_index(axis)
        for step in range(1, size):
            pl.semaphore_signal(
                barrier, inc=1, device_id={axis: lax.rem(me + step, size)}, device_id_type=MESH
            )
        total += size - 1
    pl.semaphore_wait(barrier, total)
    used = [0]
    waiting = []

    def send(source, target, axis, peer):
        slot = used[0]
        used[0] += 1
        copy = pltpu.make_async_remote_copy(
            src_ref=source,
            dst_ref=target,
            send_sem=send_sem.at[slot],
            recv_sem=recv_sem.at[slot],
            device_id={axis: peer},
            device_id_type=MESH,
        )
        copy.start()
        return copy

    relays = []
    local = []
    for index, (mode, axis) in enumerate(plan):
        source, target = sources[index], targets[index]
        size = axes[axis]
        me = lax.axis_index(axis)
        if mode == "shift":
            up, down = lax.rem(me + 1, size), lax.rem(me + size - 1, size)
            waiting.append(send(source.at[1], target.at[0], axis, up))
            waiting.append(send(source.at[0], target.at[1], axis, down))
            continue
        own = pltpu.make_async_copy(
            source.at[me] if mode == "exchange" else source, target.at[me], local_sem.at[index]
        )
        own.start()
        local.append(own)
        if mode == "relay":
            relays.append((source, target, axis))
            continue
        for step in range(1, size):
            peer = lax.rem(me + step, size)
            part = source.at[peer] if mode == "exchange" else source
            waiting.append(send(part, target.at[me], axis, peer))
    for source, target, axis in relays:
        relay(source, target, axis, axes[axis], inner, send_sem, recv_sem, used[0])
    for copy in waiting:
        copy.wait()
    for copy in local:
        copy.wait()


def communicate(name, ident, sizes, plan, *arrays):
    axes = {axis: sizes[axis] for _, axis in plan}
    inner = 1
    while (2 * inner) ** 2 <= sizes["gx"]:
        inner *= 2
    slots = 0
    shapes = []
    for (mode, axis), array in zip(plan, arrays):
        size = axes[axis]
        if mode == "shift":
            slots += 2
            shapes.append(array.shape)
        elif mode == "exchange":
            slots += size - 1
            shapes.append(array.shape)
        else:
            slots += len(relay_slots(array.shape[0], size, inner)) if mode == "relay" else size - 1
            shapes.append((size, *array.shape))
    return pl.pallas_call(
        functools.partial(comm_kernel, plan, axes, inner),
        out_shape=[jax.ShapeDtypeStruct(s, F32) for s in shapes],
        in_specs=[VMEM] * len(plan),
        out_specs=[VMEM] * len(plan),
        scratch_shapes=[
            pltpu.SemaphoreType.DMA((slots,)),
            pltpu.SemaphoreType.DMA((slots,)),
            pltpu.SemaphoreType.DMA((len(plan),)),
        ],
        compiler_params=params(collective_id=ident, has_side_effects=True),
        name=name,
    )(*arrays)


def relay_slots(fields, size, inner):
    outer = size // inner
    keys = [("own", f, 0, hop) for f in range(fields) for hop in range(1, inner)]
    for f in range(fields):
        if f < fields // 2:
            for way in ("up", "down"):
                keys += [(way, f, 0, d) for d in range(1, outer)]
                keys += [
                    (way + "x", f, hop, d) for d in range(1, outer) for hop in range(1, inner)
                ]
        else:
            for way in ("up", "down"):
                keys += [(way, f, hop, d) for d in range(1, outer) for hop in range(inner)]
    return {key: slot for slot, key in enumerate(keys)}


def relay(source, target, axis, size, inner, send_sem, recv_sem, base):
    fields = source.shape[0]
    outer = size // inner
    me = lax.axis_index(axis)
    high, low = lax.div(me, inner), lax.rem(me, inner)
    slots = relay_slots(fields, size, inner)
    has_up, has_down = high < outer - 1, high > 0
    early, late = range(fields // 2), range(fields // 2, fields)

    def place(step, hop):
        return (high - step) * inner + lax.rem(low + inner - hop, inner)

    def across(hop):
        return high * inner + lax.rem(low + hop, inner)

    def copy(key, origin, peer, own=False):
        return pltpu.make_async_remote_copy(
            src_ref=source.at[key[1]] if own else target.at[origin, key[1]],
            dst_ref=target.at[origin, key[1]],
            send_sem=send_sem.at[base + slots[key]],
            recv_sem=recv_sem.at[base + slots[key]],
            device_id={axis: peer},
            device_id_type=MESH,
        )

    finish = []

    def start(key, origin, peer, own, *conditions):
        ready = conditions[0] if conditions else None
        for more in conditions[1:]:
            ready = ready & more
        made = copy(key, origin, peer, own)
        if ready is None:
            made.start()
        else:
            pl.when(ready)(made.start)
        finish.append((made, ready))

    for f in (*late, *early):
        for hop in range(1, inner):
            start(("own", f, 0, hop), me, across(hop), True)
        start(("up", f, 0, 1), me, me + inner, True, has_up)
        start(("down", f, 0, 1), me, me - inner, True, has_down)
    for f in late:
        for hop in range(1, inner):
            origin = place(0, hop)
            copy(("own", f, 0, hop), origin, me).wait_recv()
            start(("up", f, hop, 1), origin, me + inner, False, has_up)
            start(("down", f, hop, 1), origin, me - inner, False, has_down)
    for d in range(1, outer):
        for f in range(fields):
            for hop in range(1 if f in early else inner):
                for way, sign, exists, onward in (
                    ("up", 1, high >= d, has_up),
                    ("down", -1, high + d < outer, has_down),
                ):
                    origin = place(sign * d, hop)
                    pl.when(exists)(copy((way, f, hop, d), origin, me).wait_recv)
                    if d + 1 < outer:
                        start(
                            (way, f, hop, d + 1), origin, me + sign * inner, False, exists, onward
                        )
                    if f in early:
                        for jump in range(1, inner):
                            start((way + "x", f, jump, d), origin, across(jump), False, exists)
    for f in early:
        for hop in range(1, inner):
            copy(("own", f, 0, hop), place(0, hop), me).wait_recv()
            for d in range(1, outer):
                got = copy(("upx", f, hop, d), place(d, hop), me)
                pl.when(high >= d)(got.wait_recv)
                got = copy(("downx", f, hop, d), place(-d, hop), me)
                pl.when(high + d < outer)(got.wait_recv)
    for made, ready in finish:
        if ready is None:
            made.wait_send()
        else:
            pl.when(ready)(made.wait_send)


def prepare_kernel(groups, offsets, owners, base, top, bottom, cyc, brow, bcol, frow, meta):
    fields, levels, block_x, block_y = base.shape
    row_block = lax.axis_index("gx")
    col_block = lax.axis_index("gy")
    meta[2 * groups] = row_block
    meta[2 * groups + 1] = col_block
    row_pick = jnp.full((2 * groups, block_x), -1, jnp.int32)
    col_pick = jnp.full((2 * groups + 8, block_y), -1, jnp.int32)
    row_slot = iota(row_pick.shape, 0)
    col_slot = iota(col_pick.shape, 0)
    for p in range(groups):
        g = owners[p]
        meta[2 * g] = offsets[0, p]
        meta[2 * g + 1] = offsets[1, p]
        row = offsets[0, p] - row_block * block_x
        col = offsets[1, p] - col_block * block_y
        row_pick = jnp.where(row_slot == g, row - 1, row_pick)
        row_pick = jnp.where(row_slot == g + groups, row + PC, row_pick)
        col_pick = jnp.where(col_slot == g, col - 1, col_pick)
        col_pick = jnp.where(col_slot == g + groups, col + PC, col_pick)
    col_pick = jnp.where(col_slot == 2 * groups, 0, col_pick)
    col_pick = jnp.where(col_slot == 2 * groups + 1, block_y - 1, col_pick)
    pick_rows = (iota(row_pick.shape, 1) == row_pick).astype(F32)
    pick_cols = (iota(col_pick.shape, 1) == col_pick).astype(F32)
    for z in range(levels):
        for f in range(fields):
            q = base[f, z]
            flat = z * fields + f
            found = jnp.dot(pick_rows, q, precision=HIGH, preferred_element_type=F32)
            side = lax.dot_general(
                pick_cols, q, (((1,), (1,)), ((), ())), precision=HIGH, preferred_element_type=F32
            )
            both = jnp.concatenate([side[:groups], side[groups : 2 * groups]], axis=1)
            for g in range(groups):
                high = z * 2 * fields + f
                cyc[g, high : high + 1] = found[g : g + 1]
                cyc[g, high + fields : high + fields + 1] = found[groups + g : groups + g + 1]
                at = 2 * fields * levels + flat
                cyc[g, at : at + 1] = both[g : g + 1]
            brow[0, flat : flat + 1] = q[:1]
            brow[1, flat : flat + 1] = q[block_x - 1 :]
            bcol[0, flat : flat + 1] = side[2 * groups : 2 * groups + 1]
            bcol[1, flat : flat + 1] = side[2 * groups + 1 : 2 * groups + 2]
            frow[0, flat : flat + 1] = top[f, z, 0]
            frow[1, flat : flat + 1] = bottom[f, z, 0]


def cycle_kernel(groups, fields, block_x, meta, got, piece):
    half = got.shape[1] * 2 // 3
    width = got.shape[2]
    row_block = meta[2 * groups]
    start = meta[2 * row_block]
    rows = got[0, :half]
    sides = None
    for b in range(groups):
        if b:
            rows = rows + got[b, :half]
        lane = iota((width, 2 * width), 0)
        slot = iota((width, 2 * width), 1)
        low = (lane < block_x) & (lane + b * block_x == slot + start) & (slot < PC)
        high = (
            (lane >= block_x)
            & (lane - block_x + b * block_x == slot - width + start)
            & (slot >= width)
            & (slot < width + PC)
        )
        term = jnp.dot(
            got[b, half:], (low | high).astype(F32), precision=HIGH, preferred_element_type=F32
        )
        sides = term if sides is None else sides + term
    piece[:half] = rows
    for z in range(half // (2 * fields)):
        at = half + z * 2 * fields
        piece[at : at + fields] = sides[z * fields : (z + 1) * fields, :width]
        piece[at + fields : at + 2 * fields] = sides[z * fields : (z + 1) * fields, width:]


def level(state, former, coupling, z, first, last, left, right, inverse):
    fields, levels = len(first), state(None, None)
    q = [state(f, z) for f in range(fields)]
    out = []
    for f in range(fields):
        north = jnp.concatenate([q[f][1:], last[f]], axis=0)
        south = jnp.concatenate([first[f], q[f][:-1]], axis=0)
        east = jnp.concatenate([q[f][:, 1:], right[f]], axis=1)
        west = jnp.concatenate([left[f], q[f][:, :-1]], axis=1)
        advect = (q[0] * (north - south) + q[1] * (east - west)) * (0.5 * inverse)
        laplace = (north + south + east + west - 4.0 * q[f]) * (inverse * inverse)
        upper = jnp.where(z < levels - 1, state(f, jnp.minimum(z + 1, levels - 1)), 0.0)
        lower = jnp.where(z > 0, state(f, jnp.maximum(z - 1, 0)), 0.0)
        vertical = 2.0 * q[f] - upper - lower
        coupled = coupling[f, 0] * q[0]
        for g in range(1, fields):
            coupled = coupled + coupling[f, g] * q[g]
        out.append(
            q[f]
            - former(f)
            + time_step * (advect - viscosity * laplace + vertical_mix * vertical + coupled)
        )
    return out


def fold(values):
    total = jnp.sum(values, axis=0, keepdims=True)
    acc = total[:, :128]
    for at in range(128, values.shape[1], 128):
        part = total[:, at : at + 128]
        if part.shape[1] < 128:
            part = jnp.concatenate([part, jnp.zeros((1, 128 - part.shape[1]), F32)], axis=1)
        acc = acc + part
    return acc


def fine_kernel(
    groups, members, meta, coupling, gath, halo, sums, state, old, res, rest, sq, edge, side, fit, thin, ring
):
    z = pl.program_id(0)
    fields, levels = state.shape[:2]
    fine_rows, fine_cols = state.shape[2], state.shape[4]
    piece = fine_rows // RATIO
    block_y = gath.shape[2]
    row_block = meta[2 * groups]
    col_block = meta[2 * groups + 1]
    start_y = meta[2 * row_block + 1]
    half = 2 * fields * levels

    @pl.when(z == 0)
    def _():
        sq[...] = sums[...]
        lane = iota((block_y, fine_cols), 0)
        fine = iota((block_y, fine_cols), 1) // RATIO
        rows = None
        cols = gath[0, half:]
        for b in range(members):
            pick = (lane + b * block_y == fine + start_y).astype(F32)
            term = jnp.dot(gath[b, :half], pick, precision=HIGH, preferred_element_type=F32)
            rows = term if rows is None else rows + term
            if b:
                cols = cols + gath[b, half:]
        edge[...] = rows
        pick = iota((128, 128), 0) == piece * col_block + iota((128, 128), 1) // RATIO
        side[...] = jnp.dot(cols, pick.astype(F32), precision=HIGH, preferred_element_type=F32)
        cell = iota((fine_cols, 128), 0) // RATIO + start_y
        fit[...] = (lax.rem(cell, block_y) == iota((fine_cols, 128), 1)).astype(F32).astype(BF16)

        for f in range(fields):
            ring[0, f] = state[f, 0, :, 0, :]

    @pl.when(z + 1 < levels)
    def _():
        for f in range(fields):
            ring[lax.rem(z + 1, 3), f] = state[f, z + 1, :, 0, :]

    at = pl.multiple_of(z * 2 * fields, 8)
    edges = edge[pl.ds(at, 2 * fields)]
    turned = jnp.transpose(side[pl.ds(at, 2 * fields)])
    first, last, left, right = [], [], [], []
    for f in range(fields):
        above = halo[0, pl.ds(z * fields + f, 1)]
        below = halo[1, pl.ds(z * fields + f, 1)]
        first.append(jnp.where(col_block == 0, edges[f : f + 1], above))
        last.append(jnp.where(col_block == members - 1, edges[fields + f : fields + f + 1], below))
        left.append(turned[:fine_rows, f : f + 1])
        right.append(turned[:fine_rows, fields + f : fields + f + 1])

    def cell(f, at):
        return levels if f is None else ring[lax.rem(at, 3), f]

    got = level(
        cell, lambda f: old[f, 0, :, 0, :], coupling, z, first, last, left, right, float(RATIO)
    )
    squares = None
    for f in range(fields):
        res[f, 0, :, 0, :] = got[f]
        squares = got[f] * got[f] if f == 0 else squares + got[f] * got[f]
        major = got[f].astype(BF16)
        minor = (got[f] - major.astype(F32)).astype(BF16)
        narrow = jnp.dot(major, fit[...], preferred_element_type=F32) + jnp.dot(
            minor, fit[...], preferred_element_type=F32
        )
        thin[f] = narrow * (1.0 / (RATIO * RATIO))
        total = thin[f, pl.ds(0, piece, stride=RATIO), :]
        for k in range(1, RATIO):
            total = total + thin[f, pl.ds(k, piece, stride=RATIO), :]
        rest[f, pl.ds(z, piece, stride=levels), :] = total
    sq[0:1] += fold(squares) * (1.0 / (RATIO * RATIO))


def base_kernel(groups, members, meta, coupling, rows, cols, state, old, res, sq):
    z = pl.program_id(0)
    fields, levels, block_x, block_y = state.shape
    row_block = meta[2 * groups]
    col_block = meta[2 * groups + 1]

    @pl.when(z == 0)
    def _():
        sq[...] = jnp.zeros_like(sq)

    first, last, left, right = [], [], [], []
    for f in range(fields):
        at = z * fields + f
        first.append(jnp.where(row_block > 0, rows[0, pl.ds(at, 1)], 0.0))
        last.append(jnp.where(row_block < groups - 1, rows[1, pl.ds(at, 1)], 0.0))
        left.append(jnp.where(col_block > 0, cols[0, pl.ds(at, 1)], 0.0))
        right.append(jnp.where(col_block < members - 1, cols[1, pl.ds(at, 1)], 0.0))
    turned = jnp.transpose(jnp.concatenate(left + right, axis=0))
    left = [turned[:, f : f + 1] for f in range(fields)]
    right = [turned[:, fields + f : fields + f + 1] for f in range(fields)]

    def cell(f, at):
        return levels if f is None else state[f, at]

    got = level(cell, lambda f: old[f, 0], coupling, z, first, last, left, right, 1.0)
    x = iota((block_x, block_y), 0) + row_block * block_x
    y = iota((block_x, block_y), 1) + col_block * block_y
    covered = jnp.zeros((block_x, block_y), jnp.bool_)
    for g in range(groups):
        dx, dy = x - meta[2 * g], y - meta[2 * g + 1]
        covered = covered | ((dx >= 0) & (dx < PC) & (dy >= 0) & (dy < PC))
    squares = None
    for f in range(fields):
        res[f, 0] = got[f]
        squares = got[f] * got[f] if f == 0 else squares + got[f] * got[f]
    sq[0:1] += fold(jnp.where(covered, 0.0, squares))


def sort_kernel(groups, members, block_x, meta, got, sums, slots, total):
    fields, depth, block_y = got.shape[1:]
    levels = depth * RATIO // (PC * RATIO // members)
    piece = depth // levels
    row_block = meta[2 * groups]
    col_block = meta[2 * groups + 1]
    acc = sums[0]
    for g in range(1, groups):
        acc = acc + sums[g]
    total[...] = acc
    for g in range(groups):
        begin = meta[2 * g] + col_block * piece - row_block * block_x
        start_y = meta[2 * g + 1]
        here = (begin < block_x) & (begin + piece > 0)
        for b in range(members):
            shift = start_y - b * block_y

            @pl.when(here & (shift < block_y) & (shift + PC > 0))
            def _():
                lane = iota((depth, block_y), 1)
                inside = (lane >= shift) & (lane < shift + PC)
                for f in range(fields):
                    slots[b, f] = jnp.where(inside, got[g, f], slots[b, f])


def place_kernel(groups, members, meta, tend, got, sums, out, norm, laid):
    fields, levels, block_x, block_y = tend.shape
    depth = got.shape[2]
    piece = depth // levels
    row_block = meta[2 * groups]
    col_block = meta[2 * groups + 1]
    acc = sums[0]
    for b in range(1, members):
        acc = acc + sums[b]
    norm[...] = jnp.sqrt(jnp.sum(acc, keepdims=True))
    x = iota((block_x, block_y), 0) + row_block * block_x
    y = iota((block_x, block_y), 1) + col_block * block_y
    covered = jnp.zeros((block_x, block_y), jnp.bool_)
    for g in range(groups):
        dx, dy = x - meta[2 * g], y - meta[2 * g + 1]
        covered = covered | ((dx >= 0) & (dx < PC) & (dy >= 0) & (dy < PC))
        begin = meta[2 * g] - row_block * block_x
        shift = meta[2 * g + 1] - col_block * block_y

        @pl.when((begin < block_x) & (begin + PC > 0) & (shift < block_y) & (shift + PC > 0))
        def _():
            lane = iota((levels, block_y), 1)
            inside = (lane >= shift) & (lane < shift + PC)

            def row(at, carry):
                patch_row = at - begin
                part = patch_row // piece
                source = pl.multiple_of((patch_row - part * piece) * levels, levels)
                target = pl.multiple_of(at * levels, levels)
                for f in range(fields):
                    laid[f, pl.ds(target, levels)] = jnp.where(
                        inside,
                        got[part, f, pl.ds(source, levels)],
                        laid[f, pl.ds(target, levels)],
                    )
                return carry

            lax.fori_loop(jnp.maximum(begin, 0), jnp.minimum(begin + PC, block_x), row, 0)

    for f in range(fields):
        for z in range(levels):
            out[f, z] = jnp.where(
                covered, laid[f, pl.ds(z, block_x, stride=levels), :], tend[f, z]
            )


def local(sizes, base_state, base_old, fine_state, fine_old, coupling, patch_offsets, patch_group):
    groups, members = sizes["gx"], sizes["gy"]
    fields, levels, block_x, block_y = base_state.shape
    fine_rows, fine_cols = fine_state.shape[3:]
    piece = fine_rows // RATIO
    flat = fields * levels
    def shape(*dims):
        return jax.ShapeDtypeStruct(dims, F32)

    tail = fine_rows - 1
    fine_turned = jnp.swapaxes(fine_state, 2, 3)
    cyc, brow, bcol, frow, meta = pl.pallas_call(
        functools.partial(prepare_kernel, groups),
        grid=(1,),
        out_shape=[
            shape(groups, 3 * flat, block_y),
            shape(2, flat, block_y),
            shape(2, flat, block_x),
            shape(2, flat, fine_cols),
            jax.ShapeDtypeStruct((2 * groups + 2,), jnp.int32),
        ],
        in_specs=[
            SMEM,
            SMEM,
            VMEM,
            pl.BlockSpec((fields, levels, 1, 1, fine_cols), lambda i: (0, 0, 0, 0, 0)),
            pl.BlockSpec((fields, levels, 1, 1, fine_cols), lambda i: (0, 0, tail, 0, 0)),
        ],
        out_specs=[VMEM] * 4 + [SMEM],
        compiler_params=params(),
        name="prepare",
    )(patch_offsets.T, patch_group, base_state, fine_turned, fine_turned)

    cyc, brow, bcol, frow = communicate(
        "edges",
        1,
        sizes,
        (("exchange", "gx"), ("shift", "gx"), ("shift", "gy"), ("shift", "gy")),
        cyc,
        brow,
        bcol,
        frow,
    )
    cycle = pl.pallas_call(
        functools.partial(cycle_kernel, groups, fields, block_x),
        out_shape=shape(4 * flat, block_y),
        in_specs=[SMEM, VMEM],
        out_specs=VMEM,
        compiler_params=params(),
        name="cycle",
    )(meta, cyc)
    (gath,) = communicate("members", 2, sizes, (("gather", "gy"),), cycle)

    whole = (fields, levels, block_x, block_y)
    sheet = (fields, 1, block_x, block_y)
    tend, base_sq = pl.pallas_call(
        functools.partial(base_kernel, groups, members),
        grid=(levels,),
        out_shape=[shape(*whole), shape(8, 128)],
        in_specs=[
            SMEM,
            SMEM,
            VMEM,
            VMEM,
            pl.BlockSpec(whole, lambda z: (0, 0, 0, 0)),
            pl.BlockSpec(sheet, lambda z: (0, z, 0, 0)),
        ],
        out_specs=[
            pl.BlockSpec(sheet, lambda z: (0, z, 0, 0)),
            pl.BlockSpec((8, 128), lambda z: (0, 0)),
        ],
        compiler_params=params(),
        name="base",
    )(meta, coupling, brow, bcol, base_state, base_old)

    slab = (fields, levels, fine_rows, 1, fine_cols)
    thin = (fields, 1, fine_rows, 1, fine_cols)
    fine_res, rest, fine_sq = pl.pallas_call(
        functools.partial(fine_kernel, groups, members),
        grid=(levels,),
        out_shape=[shape(*slab), shape(fields, piece * levels, 128), shape(8, 128)],
        in_specs=[
            SMEM,
            SMEM,
            VMEM,
            VMEM,
            VMEM,
            pl.BlockSpec(slab, lambda z: (0, 0, 0, 0, 0)),
            pl.BlockSpec(thin, lambda z: (0, z, 0, 0, 0)),
        ],
        out_specs=[
            pl.BlockSpec(thin, lambda z: (0, z, 0, 0, 0)),
            pl.BlockSpec((fields, piece * levels, 128), lambda z: (0, 0, 0)),
            pl.BlockSpec((8, 128), lambda z: (0, 0)),
        ],
        scratch_shapes=[
            pltpu.VMEM((2 * flat, fine_cols), F32),
            pltpu.VMEM((2 * flat, 128), F32),
            pltpu.VMEM((fine_cols, 128), BF16),
            pltpu.VMEM((fields, fine_rows, 128), F32),
            pltpu.VMEM((3, fields, fine_rows, fine_cols), F32),
        ],
        compiler_params=params(),
        name="fine",
    )(meta, coupling, gath, frow, base_sq, fine_turned, jnp.swapaxes(fine_old, 2, 3))

    gathered, sums = communicate(
        "owners", 3, sizes, (("relay", "gx"), ("gather", "gx")), rest, fine_sq
    )
    slots, total = pl.pallas_call(
        functools.partial(sort_kernel, groups, members, block_x),
        out_shape=[shape(members, fields, piece * levels, block_y), shape(8, 128)],
        in_specs=[SMEM, VMEM, VMEM],
        out_specs=[VMEM, VMEM],
        compiler_params=params(),
        name="sort",
    )(meta, gathered, sums)
    slots, sums = communicate(
        "columns", 4, sizes, (("exchange", "gy"), ("gather", "gy")), slots, total
    )
    base_out, norm = pl.pallas_call(
        functools.partial(place_kernel, groups, members),
        out_shape=[shape(*whole), shape(1, 1)],
        in_specs=[SMEM, VMEM, VMEM, VMEM],
        out_specs=[VMEM, VMEM],
        scratch_shapes=[pltpu.VMEM((fields, block_x * levels, block_y), F32)],
        compiler_params=params(),
        name="place",
    )(meta, tend, slots, sums)
    return (base_out, jnp.swapaxes(fine_res, 2, 3), norm[0, 0])


def solution(mesh):
    placed = (
        P(None, None, "gx", "gy"),
        P(None, None, "gx", "gy"),
        P(None, None, "gx", "gy", None),
        P(None, None, "gx", "gy", None),
        P(),
        P(),
        P(),
    )
    return jax.shard_map(
        functools.partial(local, dict(mesh.shape)),
        mesh=mesh,
        in_specs=placed,
        out_specs=(P(None, None, "gx", "gy"), P(None, None, "gx", "gy", None), P()),
        check_vma=False,
    )
```
